128 devices in a mesh: row: 16 (over x_hi, z, core), col: 8 (over y, x_lo).
Axes of the slice: x: 4 (x_hi: 2, x_lo: 2; x = x_hi * 2 + x_lo), y: 4, z: 4, core: 2. Of those that a mesh axis runs over, the one named last changes fastest.
Arguments:
- spins_up: int32 [10240, 16384], P('row', 'col'), may hold values from 0 to 1
- uniforms: float32 [2, 10240, 16384], P(None, 'row', 'col'), may hold values from 0 to 1
- moments: bfloat16 [10240, 16384], P('row', 'col'), may hold values from 0.5 to 2
- accept_bar: float32 [2], replicated, may hold values from 0.06 to 0.6, as said below
Outputs:
- spins_out: float32 [10240, 16384], P('row', 'col')
- corr: float32 [2048], P(('row', 'col'))
The draws below stay inside these ranges and needn't reach their ends.
Inputs may be any that keep to these rules, and one draw needn't show every extreme that they name: accept_bar[1] equals accept_bar[0] squared, as exp(-8 beta) and exp(-4 beta) for one inverse temperature beta of the draw.
All inputs are finite; a program needn't handle non-finite values.
Results may differ from the reference program's by a relative error of at most 0.0003.
Values may be sent and summed in bfloat16 or wider, within the bound.
A program may use at most 128 MiB of HBM per device.

```python
import math
import jax
import jax.numpy as jnp
from jax import lax

ROWS = 640
CB = 2048
R = 2048
SWEEPS = 2
NR = 10240
NC = 16384


def draw_accept_bar(key, part):
    chosen = jax.random.fold_in(key, 17)
    accept_four = jax.random.uniform(chosen, (), jnp.float32, 0.25, 0.6)
    return jnp.stack([accept_four, accept_four * accept_four]).astype(jnp.float32)


def band_bits(key, length, narrow, widest, offset_top):
    width_key, phase_key, value_key = jax.random.split(key, 3)
    band_count = (length + offset_top) // narrow + 1
    widths = jax.random.randint(width_key, (band_count,), narrow, widest + 1)
    ends = jnp.cumsum(widths)
    phase = jax.random.randint(phase_key, (), 0, offset_top + 1)
    places = jnp.arange(length, dtype=jnp.int32) + phase
    band_ids = jnp.sum((places[:, None] >= ends[None, :]).astype(jnp.int32), axis=1)
    values = jax.random.randint(value_key, (band_count + 1,), 0, 2)
    return values[band_ids]


def draw_spins_up(key, part):
    base = jax.random.fold_in(key, 29)
    column_key, row_key, noise_key = jax.random.split(base, 3)
    column_narrow = max(CB // 32, 2)
    column_bits = band_bits(column_key, NC, column_narrow, 2 * CB, 2 * CB)
    row_narrow = max(ROWS // 8, 2)
    row_bits = band_bits(row_key, NR, row_narrow, 2 * ROWS, 2 * ROWS)
    noise = (jax.random.randint(noise_key, (NR, NC), 0, 10) == 0).astype(jnp.int32)
    return ((row_bits[:, None] + column_bits[None, :] + noise) % 2).astype(jnp.int32)


def shard_levels(rng, shape, shards, least, largest):
    def one(axis_at, shards_of):
        heights = jax.random.uniform(jax.random.fold_in(jax.random.fold_in(rng, 6), axis_at), (shards_of,), jnp.float32, least / len(shards), largest / len(shards))
        return jnp.repeat(jnp.exp(heights), shape[axis_at] // shards_of).reshape((-1,) + (1,) * (len(shape) - axis_at - 1))

    level = one(*shards[0])
    for cut in shards[1:]:
        level = level * one(*cut)
    return level


def setup_inputs(seed: int = 0) -> dict:
    arg_keys = jax.random.split(jax.random.key(seed), 5)
    return {
        "spins_up": draw_spins_up(jax.random.fold_in(arg_keys[4], 71), 0),
        "uniforms": jnp.clip(1.0 * jax.random.uniform(arg_keys[1], (SWEEPS, NR, NC), jnp.float32) ** shard_levels(arg_keys[1], (SWEEPS, NR, NC), ((1, 16), (2, 8)), -0.2, 0.2), 0.0, 1.0),
        "moments": jnp.clip(jnp.exp(math.log(2.0) - 1.3862944 * jax.random.uniform(arg_keys[2], (NR, NC), jnp.float32) ** shard_levels(arg_keys[2], (NR, NC), ((0, 16), (1, 8)), -0.2, 0.2)), 0.5, 2.0).astype(jnp.bfloat16),
        "accept_bar": draw_accept_bar(jax.random.fold_in(arg_keys[4], 71), 0),
    }


def update_colour(lattice, uniform_draws, accept_bar, colour):
    neighbours = jnp.roll(lattice, 1, 0) + jnp.roll(lattice, -1, 0) + jnp.roll(lattice, 1, 1) + jnp.roll(lattice, -1, 1)
    alignment = lattice * neighbours
    threshold = jnp.where(alignment > 3.0, accept_bar[1], accept_bar[0])
    row_ids = lax.broadcasted_iota(jnp.int32, lattice.shape, 0)
    col_ids = lax.broadcasted_iota(jnp.int32, lattice.shape, 1)
    coloured = (row_ids + col_ids) % 2 == colour
    flipped = coloured & ((alignment <= 0.0) | (uniform_draws < threshold))
    return jnp.where(flipped, -lattice, lattice)

def reference(spins_up, uniforms, moments, accept_bar):
    lattice = (2 * spins_up - 1).astype(jnp.float32)
    for sweep_index in range(SWEEPS):
        for colour in range(2):
            lattice = update_colour(lattice, uniforms[sweep_index], accept_bar, colour)
    weighted = (moments * lattice.astype(jnp.bfloat16)).astype(jnp.float32)
    strips = weighted.reshape(NR // ROWS, ROWS, NC)

    def strip_corr(strip_rows):
        spectrum = jnp.fft.rfft(strip_rows, axis=1)
        power_sum = spectrum.real * spectrum.real + spectrum.imag * spectrum.imag
        circular = jnp.fft.irfft(power_sum, n=NC, axis=1)
        return lax.optimization_barrier(jnp.sum(circular[:, :R], axis=0))
    partials = lax.map(strip_corr, strips)
    normaliser = 1.0 / math.sqrt(NR * NC)
    corr = (lax.optimization_barrier(jnp.sum(partials, axis=0)) * normaliser).astype(jnp.float32)
    return (lattice, corr)
```

```python
import math

import jax
import jax.numpy as jnp
from jax import lax
from jax.experimental import pallas as pl
from jax.experimental.pallas import tpu as pltpu
from jax.sharding import PartitionSpec as P

ROWS = 640
CB = 2048
R = 2048
NROW = 16
NCOL = 8
HALO = 8
UNIT = 64
CHUNKS = 5
WIDE = CB + 128
TILE = 256
MESH = pl.DeviceIdType.MESH


def kernel(
    su_hbm, u_hbm, m_hbm, bar, w_hbm, corr_ref,
    su, u, m, ht, wk, wn, buf, lt, prod, fold, outbox, inbox, vb, rs1, rs2, sb,
    edge_sem, u_sem, s_sem, m_sem, w_sem, col_send, col_recv,
    row_send, row_recv, ys, yr, xs, xr, r1s, r1r, r2s, r2r,
):
    f32, bf16 = jnp.float32, jnp.bfloat16
    row = lax.axis_index("row")
    col = lax.axis_index("col")
    par = lax.rem(col, 2)
    xcol = col + 1 - 2 * par
    ycol = lax.rem(col + 6 + 4 * par, NCOL)
    left, right = lax.rem(col + NCOL - 1, NCOL), lax.rem(col + 1, NCOL)
    up, down = lax.rem(row + NROW - 1, NROW), lax.rem(row + 1, NROW)
    own = 16 * par
    far = 16 * (1 - par)

    barrier = pltpu.get_barrier_semaphore()
    for i in range(1, NROW):
        pl.semaphore_signal(
            barrier, inc=1, device_id=(lax.rem(row + i, NROW), col), device_id_type=MESH
        )
    for i in range(1, NCOL):
        pl.semaphore_signal(
            barrier, inc=1, device_id=(row, lax.rem(col + i, NCOL)), device_id_type=MESH
        )

    def edge_copies():
        out = []
        for e, lo in enumerate((0, CB - 128)):
            lanes = pl.ds(lo, 128)
            out.append(pltpu.make_async_copy(
                u_hbm.at[:, :, lanes], u.at[:, pl.ds(HALO, ROWS), lanes], edge_sem.at[2 * e]))
            out.append(pltpu.make_async_copy(
                su_hbm.at[:, lanes], su.at[pl.ds(HALO, ROWS), lanes], edge_sem.at[2 * e + 1]))
        return out

    inner = pl.ds(128, CB - 256)

    def piece_copies(j):
        at = pl.multiple_of(j * UNIT, UNIT)
        to = pl.multiple_of(j * UNIT + HALO, 8)
        return (
            pltpu.make_async_copy(
                u_hbm.at[:, pl.ds(at, UNIT), inner], u.at[:, pl.ds(to, UNIT), inner], u_sem.at[j]),
            pltpu.make_async_copy(
                su_hbm.at[pl.ds(at, UNIT), inner], su.at[pl.ds(to, UNIT), inner], s_sem.at[j]),
            pltpu.make_async_copy(
                m_hbm.at[pl.ds(at, UNIT), :], m.at[pl.ds(at, UNIT), :], m_sem.at[j]),
        )

    for cp in edge_copies():
        cp.start()
    for j in (4, 3, 5):
        for cp in piece_copies(j):
            cp.start()

    a0 = bar[0]
    a1 = bar[1]

    def limit(draws):
        return jnp.where(draws < a1, 4.0, jnp.where(draws < a0, 2.0, 0.0)).astype(f32)

    def select(side, k):
        r = lax.broadcasted_iota(jnp.int32, (16, 128), 0)
        c = lax.broadcasted_iota(jnp.int32, (16, 128), 1)
        c = c - 124 * side
        hit = (c >= 0) & (c < 4) & (r == 4 * k + c)
        return jnp.where(hit, 1.0, 0.0).astype(bf16)

    wk[0:8, :] = jnp.zeros((8, WIDE), f32)
    wk[88:96, :] = jnp.zeros((8, WIDE), f32)
    for cp in edge_copies():
        cp.wait()

    def pack_edges(b, carry):
        r = pl.multiple_of(HALO + 128 * b, 8)
        dst = pl.ds(pl.multiple_of(128 * b, 128), 128)
        for side in range(2):
            lanes = pl.ds(side * (CB - 128), 128)
            parts = (
                (2 * su[pl.ds(r, 128), lanes] - 1).astype(f32),
                limit(u[0, pl.ds(r, 128), lanes]),
                limit(u[1, pl.ds(r, 128), lanes]),
            )
            msg = jnp.zeros((16, 128), f32)
            for k, x in enumerate(parts):
                msg = msg + lax.dot_general(
                    select(side, k), x.astype(bf16), (((1,), (1,)), ((), ())),
                    preferred_element_type=f32)
            outbox[side, :, dst] = msg.astype(bf16)
        return carry

    lax.fori_loop(0, 5, pack_edges, 0)

    pl.semaphore_wait(barrier, NROW + NCOL - 2)

    def col_copy(side):
        return pltpu.make_async_remote_copy(
            src_ref=outbox.at[side], dst_ref=inbox.at[side],
            send_sem=col_send.at[side], recv_sem=col_recv.at[side],
            device_id=(row, left if side == 0 else right), device_id_type=MESH)

    for side in range(2):
        col_copy(side).start()

    def row_copies(side):
        dev = (down if side == 0 else up, col)
        src_at = ROWS - HALO if side == 0 else 0
        dst_at = 0 if side == 0 else ROWS + HALO
        return (
            pltpu.make_async_remote_copy(
                src_ref=u_hbm.at[:, pl.ds(src_at, HALO), :], dst_ref=u.at[:, pl.ds(dst_at, HALO), :],
                send_sem=row_send.at[3 * side], recv_sem=row_recv.at[3 * side],
                device_id=dev, device_id_type=MESH),
            pltpu.make_async_remote_copy(
                src_ref=su_hbm.at[pl.ds(src_at, HALO), :], dst_ref=su.at[pl.ds(dst_at, HALO), :],
                send_sem=row_send.at[3 * side + 1], recv_sem=row_recv.at[3 * side + 1],
                device_id=dev, device_id_type=MESH),
        )

    def halo_tile_copy(side):
        dev = (down if side == 0 else up, col)
        src_at = ROWS if side == 0 else HALO
        dst_at = 0 if side == 0 else ROWS + HALO
        return pltpu.make_async_remote_copy(
            src_ref=ht.at[:, pl.ds(src_at, HALO), :], dst_ref=ht.at[:, pl.ds(dst_at, HALO), :],
            send_sem=row_send.at[3 * side + 2], recv_sem=row_recv.at[3 * side + 2],
            device_id=dev, device_id_type=MESH)

    for side in range(2):
        for cp in row_copies(side):
            cp.start()
    for j in (6, 2, 7, 1, 8, 0, 9):
        for cp in piece_copies(j):
            cp.start()

    def clear(o, carry):
        prod[o] = jnp.zeros((TILE, TILE), f32)
        return carry

    lax.fori_loop(0, 9, clear, 0)

    for side in range(2):
        col_copy(side).wait_recv()

    def unpack_edges(b, carry):
        r = pl.multiple_of(HALO + 128 * b, 8)
        src = pl.ds(pl.multiple_of(128 * b, 128), 128)
        for k in range(3):
            tile = jnp.zeros((128, 128), f32)
            for side in range(2):
                tile = tile + lax.dot_general(
                    inbox[side, :, src], select(side, k), (((0,), (0,)), ((), ())),
                    preferred_element_type=f32)
            ht[k, pl.ds(r, 128), :] = tile
        return carry

    lax.fori_loop(0, 5, unpack_edges, 0)
    for side in range(2):
        halo_tile_copy(side).start()

    def y_copy(c):
        return pltpu.make_async_remote_copy(
            src_ref=buf.at[c, pl.ds(own, 8)], dst_ref=buf.at[c, pl.ds(far, 8)],
            send_sem=ys.at[c], recv_sem=yr.at[c],
            device_id=(row, ycol), device_id_type=MESH)

    def x_copy(c):
        return pltpu.make_async_remote_copy(
            src_ref=buf.at[c, pl.ds(24, 8)], dst_ref=buf.at[c, pl.ds(8, 8)],
            send_sem=xs.at[c], recv_sem=xr.at[c],
            device_id=(row, xcol), device_id_type=MESH)

    def w_copy(j):
        at = pl.multiple_of(j * UNIT, UNIT)
        return pltpu.make_async_copy(
            wn.at[pl.ds(at, UNIT), :], w_hbm.at[pl.ds(at, UNIT), :], w_sem.at[j])

    sub = lax.broadcasted_iota(jnp.int32, (8, WIDE), 0)
    parity = lax.rem(sub + lax.broadcasted_iota(jnp.int32, (8, WIDE), 1), 2)

    for j in (4, 3):
        for cp in piece_copies(j)[:2]:
            cp.wait()

    def unit(k, carry):
        odd = lax.rem(k, 2)
        c = lax.div(k, 2)
        j = (4 - c) * (1 - odd) + (5 + c) * odd
        keep = 1 - lax.rem(k + par, 2)
        row0 = j * UNIT
        more = j + 2 * odd - 1 + 2 * jnp.maximum(1 - k, 0)

        @pl.when(k < 8)
        def _():
            for cp in piece_copies(more)[:2]:
                cp.wait()

        for side in range(2):
            @pl.when(k == 8 + side)
            def _():
                for cp in row_copies(side):
                    cp.wait_recv()
                halo_tile_copy(side).wait_recv()

        piece_copies(j)[2].wait()

        def fill(g, carry):
            r = pl.multiple_of(8 * g, 8)
            e = pl.multiple_of(row0 + 8 * g, 8)
            wk[pl.ds(r + 8, 8), 0:CB] = (2 * su[pl.ds(e, 8), :] - 1).astype(f32)
            wk[pl.ds(r + 8, 8), CB:WIDE] = ht[0, pl.ds(e, 8), :]
            return carry

        lax.fori_loop(0, 10, fill, 0)

        def half(h, carry):
            sweep = lax.div(h, 2)
            coloured = parity == lax.rem(h, 2)

            def group(g, carry):
                r = pl.multiple_of(8 * g, 8)
                e = pl.multiple_of(row0 + 8 * g, 8)
                before = wk[pl.ds(r, 8), :]
                cur = wk[pl.ds(r + 8, 8), :]
                after = wk[pl.ds(r + 16, 8), :]
                near = (
                    pltpu.roll(jnp.where(sub == 7, before, cur), 1, 0)
                    + pltpu.roll(jnp.where(sub == 0, after, cur), 7, 0)
                    + pltpu.roll(cur, 1, 1)
                    + pltpu.roll(cur, WIDE - 1, 1)
                )
                bound = jnp.concatenate(
                    [limit(u[sweep, pl.ds(e, 8), :]), ht[1 + sweep, pl.ds(e, 8), :]], axis=1)
                flip = coloured & (cur * near <= bound)
                wk[pl.ds(r + 8, 8), :] = jnp.where(flip, -cur, cur)
                return carry

            lax.fori_loop(0, 10, group, 0)
            return carry

        lax.fori_loop(0, 4, half, 0)

        base = own * keep + 24 * (1 - keep)

        def weigh(g, carry):
            r = pl.multiple_of(16 * g, 16)
            a = pl.multiple_of(row0 + 16 * g, 16)
            w = m[pl.ds(a, 16), :] * wk[pl.ds(r + 16, 16), 0:CB].astype(bf16)
            for t in range(8):
                buf[c, base + t, pl.ds(r, 16), :] = w[:, TILE * t:TILE * (t + 1)]
            wn[pl.ds(a, 16), :] = w
            return carry

        lax.fori_loop(0, 4, weigh, 0)

        @pl.when(keep == 1)
        def _():
            y_copy(c).start()

        @pl.when(keep == 0)
        def _():
            x_copy(c).start()

        w_copy(j).start()
        return carry

    lax.fori_loop(0, 10, unit, 0)

    def chunk(c, carry):
        y_copy(c).wait_recv()
        x_copy(c).wait_recv()
        for t in range(8):
            rows2 = buf[c, 2 * t:2 * t + 2].reshape(128, TILE)
            lt[:, 128 * t:128 * (t + 1)] = rows2.T

        def offset(o, carry):
            rhs = buf[c, pl.ds(o, 16)].reshape(16 * UNIT, TILE)
            prod[o] += jnp.dot(lt[...], rhs, preferred_element_type=f32)
            return carry

        lax.fori_loop(0, 9, offset, 0)
        return carry

    lax.fori_loop(0, CHUNKS, chunk, 0)

    def fold_128(b, carry):
        r = pl.multiple_of(8 * b, 8)
        lo = jnp.concatenate([prod[o, pl.ds(r, 8), :] for o in range(9)], axis=1)
        hi = jnp.concatenate([prod[o, pl.ds(r + 128, 8), :] for o in range(9)], axis=1)
        fold[pl.ds(r, 8), :] = lo[:, 0:WIDE] + hi[:, 128:128 + WIDE]
        return carry

    lax.fori_loop(0, 16, fold_128, 0)
    for n in (64, 32, 16, 8):
        def fold_n(b, carry, n=n):
            r = pl.multiple_of(8 * b, 8)
            fold[pl.ds(r, 8), :] += pltpu.roll(fold[pl.ds(r + n, 8), :], WIDE - n, 1)
            return carry

        lax.fori_loop(0, n // 8, fold_n, 0)
    v = fold[0:8, :]
    for n in (4, 2, 1):
        v = v + pltpu.roll(pltpu.roll(v, WIDE - n, 1), 8 - n, 0)

    for i in range(NROW):
        vb[i] = v[0:1, 128 * i:128 * (i + 1)]

    def r1_copy(i):
        to = lax.rem(row + i, NROW)
        return pltpu.make_async_remote_copy(
            src_ref=vb.at[to], dst_ref=rs1.at[i], send_sem=r1s.at[i], recv_sem=r1r.at[i],
            device_id=(to, col), device_id_type=MESH)

    for i in range(1, NROW):
        r1_copy(i).start()
    total = vb[row]
    for i in range(1, NROW):
        r1_copy(i).wait_recv()
        total = total + rs1[i]
    sb[...] = total

    def r2_copy(i):
        return pltpu.make_async_remote_copy(
            src_ref=sb, dst_ref=rs2.at[i], send_sem=r2s.at[i], recv_sem=r2r.at[i],
            device_id=(row, lax.rem(col + i, NCOL)), device_id_type=MESH)

    for i in range(1, NCOL):
        r2_copy(i).start()
    for i in range(1, NCOL):
        r2_copy(i).wait_recv()
        total = total + rs2[i]
    total = total * (1.0 / math.sqrt(ROWS * NROW * CB * NCOL))
    total = pltpu.roll(jnp.broadcast_to(total, (8, 128)), lax.rem(128 - 16 * col, 128), 1)
    corr_ref[...] = total

    for side in range(2):
        col_copy(side).wait_send()
        for cp in row_copies(side):
            cp.wait_send()
        halo_tile_copy(side).wait_send()

    def drain(c, carry):
        y_copy(c).wait_send()
        x_copy(c).wait_send()
        w_copy(2 * c).wait()
        w_copy(2 * c + 1).wait()
        return carry

    lax.fori_loop(0, CHUNKS, drain, 0)
    for i in range(1, NROW):
        r1_copy(i).wait_send()
    for i in range(1, NCOL):
        r2_copy(i).wait_send()


def on_device(spins_up, uniforms, moments, accept_bar):
    f32, bf16 = jnp.float32, jnp.bfloat16
    vmem, dma = pltpu.VMEM, pltpu.SemaphoreType.DMA
    hbm = pl.BlockSpec(memory_space=pl.ANY)
    weighted, corr = pl.pallas_call(
        kernel,
        out_shape=(
            jax.ShapeDtypeStruct((ROWS, CB), bf16),
            jax.ShapeDtypeStruct((8, 128), f32),
        ),
        in_specs=[hbm, hbm, hbm, pl.BlockSpec(memory_space=pltpu.SMEM)],
        out_specs=(hbm, pl.BlockSpec(memory_space=pltpu.VMEM)),
        scratch_shapes=[
            vmem((ROWS + 16, CB), jnp.int32),
            vmem((2, ROWS + 16, CB), f32),
            vmem((ROWS, CB), bf16),
            vmem((3, ROWS + 16, 128), f32),
            vmem((UNIT + 32, WIDE), f32),
            vmem((ROWS, CB), bf16),
            vmem((CHUNKS, 32, UNIT, TILE), bf16),
            vmem((TILE, 16 * UNIT), bf16),
            vmem((9, TILE, TILE), f32),
            vmem((128, WIDE), f32),
            vmem((2, 16, ROWS), bf16),
            vmem((2, 16, ROWS), bf16),
            vmem((NROW, 1, 128), f32),
            vmem((NROW, 1, 128), f32),
            vmem((NCOL, 1, 128), f32),
            vmem((1, 128), f32),
            dma((4,)), dma((10,)), dma((10,)), dma((10,)), dma((10,)),
            dma((2,)), dma((2,)), dma((6,)), dma((6,)),
            dma((CHUNKS,)), dma((CHUNKS,)), dma((CHUNKS,)), dma((CHUNKS,)),
            dma((NROW,)), dma((NROW,)), dma((NCOL,)), dma((NCOL,)),
        ],
        compiler_params=pltpu.CompilerParams(
            collective_id=0, has_side_effects=True, vmem_limit_bytes=56 * 1024 * 1024,
        ),
    )(spins_up, uniforms, moments, accept_bar)
    lattice = jnp.where(weighted > 0, 1.0, -1.0).astype(f32)
    return lattice, corr[0, :16]


def solution(mesh):
    placed = (P("row", "col"), P(None, "row", "col"), P("row", "col"), P())
    return jax.shard_map(
        on_device,
        mesh=mesh,
        in_specs=placed,
        out_specs=(P("row", "col"), P(("row", "col"))),
        check_vma=False,
    )
```

```python
import math

import jax
import jax.numpy as jnp
from jax import lax
from jax.experimental import pallas as pl
from jax.experimental.pallas import tpu as pltpu
from jax.sharding import PartitionSpec as P

ROWS = 640
CB = 2048
R = 2048
NROW = 16
NCOL = 8
HALO = 8
UNIT = 64
CHUNKS = 5
WIDE = CB + 128
TILE = 256
LT = CB // 128
EDGES = (0, LT - 1)
BANDS = ((184, 272), (0, 184), (456, 184), (0, 640))
SPAN = (UNIT + 2 * HALO) // 8
PAIRS = SPAN // 2
MESH = pl.DeviceIdType.MESH


def kernel(
    su_hbm, u_hbm, m_hbm, bar, w_hbm, corr_ref,
    su, u, hu, hs, m, ht, c0, c1, wk, wn, buf, lt, prod, fold, outbox, inbox, vb, rs1, rs2, sb,
    u_sem, s_sem, m_sem, w_sem, col_send, col_recv,
    row_send, row_recv, ys, yr, xs, xr, r1s, r1r, r2s, r2r,
):
    f32, bf16 = jnp.float32, jnp.bfloat16
    row = lax.axis_index("row")
    col = lax.axis_index("col")
    par = lax.rem(col, 2)
    xcol = col + 1 - 2 * par
    ycol = lax.rem(col + 6 + 4 * par, NCOL)
    left, right = lax.rem(col + NCOL - 1, NCOL), lax.rem(col + 1, NCOL)
    up, down = lax.rem(row + NROW - 1, NROW), lax.rem(row + 1, NROW)
    own = 16 * par
    far = 16 * (1 - par)

    barrier = pltpu.get_barrier_semaphore()
    for i in range(1, NROW):
        pl.semaphore_signal(
            barrier, inc=1, device_id=(lax.rem(row + i, NROW), col), device_id_type=MESH
        )
    for i in range(1, NCOL):
        pl.semaphore_signal(
            barrier, inc=1, device_id=(row, lax.rem(col + i, NCOL)), device_id_type=MESH
        )

    def tile_copies(t, band):
        at, size = BANDS[band]
        lanes = pl.ds(128 * t, 128)
        return (
            pltpu.make_async_copy(
                u_hbm.at[:, pl.ds(at, size), lanes],
                u.at[:, t, pl.ds(at + HALO, size), :], u_sem.at[band, t]),
            pltpu.make_async_copy(
                su_hbm.at[pl.ds(at, size), lanes],
                su.at[t, pl.ds(at + HALO, size), :], s_sem.at[band, t]),
        )

    def m_copy(j):
        at = pl.multiple_of(j * UNIT, UNIT)
        return pltpu.make_async_copy(
            m_hbm.at[pl.ds(at, UNIT), :], m.at[pl.ds(at, UNIT), :], m_sem.at[j])

    def start_band(band):
        tiles = EDGES if band == 3 else range(1, LT - 1)
        for t in tiles:
            for cp in tile_copies(t, band):
                cp.start()

    def wait_band(band):
        tiles = EDGES if band == 3 else range(1, LT - 1)
        for t in tiles:
            for cp in tile_copies(t, band):
                cp.wait()

    start_band(3)
    start_band(0)

    a0 = bar[0]
    a1 = bar[1]

    def limit(draws):
        return jnp.where(draws < a1, 4.0, jnp.where(draws < a0, 2.0, 0.0)).astype(f32)

    def select(side, k):
        r = lax.broadcasted_iota(jnp.int32, (16, 128), 0)
        c = lax.broadcasted_iota(jnp.int32, (16, 128), 1)
        c = c - 124 * side
        hit = (c >= 0) & (c < 4) & (r == 4 * k + c)
        return jnp.where(hit, 1.0, 0.0).astype(bf16)

    wait_band(3)

    def pack_edges(b, carry):
        r = pl.multiple_of(HALO + 128 * b, 8)
        dst = pl.ds(pl.multiple_of(128 * b, 128), 128)
        for side in range(2):
            t = EDGES[side]
            parts = (
                (2 * su[t, pl.ds(r, 128), :] - 1).astype(f32),
                limit(u[0, t, pl.ds(r, 128), :]),
                limit(u[1, t, pl.ds(r, 128), :]),
            )
            msg = jnp.zeros((16, 128), f32)
            for k, x in enumerate(parts):
                msg = msg + lax.dot_general(
                    select(side, k), x.astype(bf16), (((1,), (1,)), ((), ())),
                    preferred_element_type=f32)
            outbox[side, :, dst] = msg.astype(bf16)
        return carry

    lax.fori_loop(0, 5, pack_edges, 0)

    pl.semaphore_wait(barrier, NROW + NCOL - 2)

    def col_copy(side):
        return pltpu.make_async_remote_copy(
            src_ref=outbox.at[side], dst_ref=inbox.at[side],
            send_sem=col_send.at[side], recv_sem=col_recv.at[side],
            device_id=(row, left if side == 0 else right), device_id_type=MESH)

    for side in range(2):
        col_copy(side).start()

    def row_copies(side):
        dev = (down if side == 0 else up, col)
        src_at = ROWS - HALO if side == 0 else 0
        return (
            pltpu.make_async_remote_copy(
                src_ref=u_hbm.at[:, pl.ds(src_at, HALO), :], dst_ref=hu.at[side],
                send_sem=row_send.at[3 * side], recv_sem=row_recv.at[3 * side],
                device_id=dev, device_id_type=MESH),
            pltpu.make_async_remote_copy(
                src_ref=su_hbm.at[pl.ds(src_at, HALO), :], dst_ref=hs.at[side],
                send_sem=row_send.at[3 * side + 1], recv_sem=row_recv.at[3 * side + 1],
                device_id=dev, device_id_type=MESH),
        )

    def halo_tile_copy(side):
        dev = (down if side == 0 else up, col)
        src_at = ROWS if side == 0 else HALO
        dst_at = 0 if side == 0 else ROWS + HALO
        return pltpu.make_async_remote_copy(
            src_ref=ht.at[:, pl.ds(src_at, HALO), :], dst_ref=ht.at[:, pl.ds(dst_at, HALO), :],
            send_sem=row_send.at[3 * side + 2], recv_sem=row_recv.at[3 * side + 2],
            device_id=dev, device_id_type=MESH)

    for side in range(2):
        for cp in row_copies(side):
            cp.start()
    for j in (4, 5, 3, 6):
        m_copy(j).start()
    for band in (1, 2):
        start_band(band)
    for j in (2, 7, 1, 8, 0, 9):
        m_copy(j).start()

    def clear(o, carry):
        prod[o] = jnp.zeros((TILE, TILE), f32)
        return carry

    lax.fori_loop(0, 9, clear, 0)

    for side in range(2):
        col_copy(side).wait_recv()

    def unpack_edges(b, carry):
        r = pl.multiple_of(HALO + 128 * b, 8)
        src = pl.ds(pl.multiple_of(128 * b, 128), 128)
        for k in range(3):
            tile = jnp.zeros((128, 128), f32)
            for side in range(2):
                tile = tile + lax.dot_general(
                    inbox[side, :, src], select(side, k), (((0,), (0,)), ((), ())),
                    preferred_element_type=f32)
            ht[k, pl.ds(r, 128), :] = tile
        return carry

    lax.fori_loop(0, 5, unpack_edges, 0)
    for side in range(2):
        halo_tile_copy(side).start()

    def y_copy(c):
        return pltpu.make_async_remote_copy(
            src_ref=buf.at[c, pl.ds(own, 8)], dst_ref=buf.at[c, pl.ds(far, 8)],
            send_sem=ys.at[c], recv_sem=yr.at[c],
            device_id=(row, ycol), device_id_type=MESH)

    def x_copy(c):
        return pltpu.make_async_remote_copy(
            src_ref=buf.at[c, pl.ds(24, 8)], dst_ref=buf.at[c, pl.ds(8, 8)],
            send_sem=xs.at[c], recv_sem=xr.at[c],
            device_id=(row, xcol), device_id_type=MESH)

    def w_copy(j):
        at = pl.multiple_of(j * UNIT, UNIT)
        return pltpu.make_async_copy(
            wn.at[pl.ds(at, UNIT), :], w_hbm.at[pl.ds(at, UNIT), :], w_sem.at[j])

    lane = lax.broadcasted_iota(jnp.int32, (8, 128), 1)
    even = lax.rem(lane, 2) == 0
    first, last = lane == 0, lane == 127
    colours = (c0, c1)

    def wrap(ref):
        for t in range(LT + 1):
            ref[0, t] = pltpu.roll(ref[PAIRS, t], 1, 0)
            ref[PAIRS + 1, t] = pltpu.roll(ref[1, t], 7, 0)

    wait_band(0)

    def unit(k, carry):
        odd = lax.rem(k, 2)
        c = lax.div(k, 2)
        j = (4 - c) * (1 - odd) + (5 + c) * odd
        keep = 1 - lax.rem(k + par, 2)
        row0 = j * UNIT

        for side in range(2):
            @pl.when(k == 4 + side)
            def _():
                wait_band(1 + side)

            @pl.when(k == 8 + side)
            def _():
                for cp in row_copies(side):
                    cp.wait_recv()
                halo_tile_copy(side).wait_recv()
                at = 0 if side == 0 else ROWS + HALO
                for t in range(LT):
                    lanes = pl.ds(128 * t, 128)
                    su[t, at:at + HALO, :] = hs[side, :, lanes]
                    for n in range(2):
                        u[n, t, at:at + HALO, :] = hu[side, n, :, lanes]

        m_copy(j).wait()

        def fill(g, carry):
            upper = pl.ds(row0 + 2 * g, 8, stride=SPAN)
            lower = pl.ds(row0 + 2 * g + 1, 8, stride=SPAN)
            for t in range(LT + 1):
                if t < LT:
                    a = (2 * su[t, upper, :] - 1).astype(f32)
                    b = (2 * su[t, lower, :] - 1).astype(f32)
                else:
                    a, b = ht[0, upper, :], ht[0, lower, :]
                c0[g + 1, t] = jnp.where(even, a, b)
                c1[g + 1, t] = jnp.where(even, b, a)
            return carry

        lax.fori_loop(0, PAIRS, fill, 0)
        wrap(c1)

        for h in range(4):
            sweep, colour = h // 2, h % 2
            mine, other = colours[colour], colours[1 - colour]

            def group(g, carry):
                upper = pl.ds(row0 + 2 * g + colour, 8, stride=SPAN)
                lower = pl.ds(row0 + 2 * g + 1 - colour, 8, stride=SPAN)
                mid = [other[g + 1, t] for t in range(LT + 1)]
                east = [pltpu.roll(x, 1, 1) for x in mid]
                west = [pltpu.roll(x, 127, 1) for x in mid]
                for t in range(LT + 1):
                    above, below = other[g, t], other[g + 2, t]
                    outer = jnp.where(even, above, below) if colour == 0 else jnp.where(even, below, above)
                    side = (jnp.where(first, east[t - 1], east[t])
                            + jnp.where(last, west[(t + 1) % (LT + 1)], west[t]))
                    if t < LT:
                        bound = limit(jnp.where(even, u[sweep, t, upper, :], u[sweep, t, lower, :]))
                    else:
                        bound = jnp.where(even, ht[1 + sweep, upper, :], ht[1 + sweep, lower, :])
                    cur = mine[g + 1, t]
                    flip = cur * (mid[t] + outer + side) <= bound
                    mine[g + 1, t] = jnp.where(flip, -cur, cur)
                return carry

            lax.fori_loop(0, PAIRS, group, 0)
            if h < 3:
                wrap(mine)

        def spread(g, carry):
            for t in range(LT):
                a, b = c0[g + 1, t], c1[g + 1, t]
                wk[t, pl.ds(2 * g, 8, stride=SPAN), :] = jnp.where(even, a, b)
                wk[t, pl.ds(2 * g + 1, 8, stride=SPAN), :] = jnp.where(even, b, a)
            return carry

        lax.fori_loop(0, PAIRS, spread, 0)
        base = own * keep + 24 * (1 - keep)

        def weigh(g, carry):
            r = pl.multiple_of(16 * g, 16)
            a = pl.multiple_of(row0 + 16 * g, 16)
            for t in range(LT):
                lanes = pl.ds(128 * t, 128)
                w = m[pl.ds(a, 16), lanes] * wk[t, pl.ds(r + 8, 16), :].astype(bf16)
                buf[c, base + t // 2, pl.ds(r, 16), 128 * (t % 2):128 * (t % 2 + 1)] = w
                wn[pl.ds(a, 16), lanes] = w
            return carry

        lax.fori_loop(0, 4, weigh, 0)

        @pl.when(keep == 1)
        def _():
            y_copy(c).start()

        @pl.when(keep == 0)
        def _():
            x_copy(c).start()

        w_copy(j).start()
        return carry

    lax.fori_loop(0, 10, unit, 0)

    def chunk(c, carry):
        y_copy(c).wait_recv()
        x_copy(c).wait_recv()
        for t in range(8):
            rows2 = buf[c, 2 * t:2 * t + 2].reshape(128, TILE)
            lt[:, 128 * t:128 * (t + 1)] = rows2.T

        def offset(o, carry):
            rhs = buf[c, pl.ds(o, 16)].reshape(16 * UNIT, TILE)
            prod[o] += jnp.dot(lt[...], rhs, preferred_element_type=f32)
            return carry

        lax.fori_loop(0, 9, offset, 0)
        return carry

    lax.fori_loop(0, CHUNKS, chunk, 0)

    def fold_128(b, carry):
        r = pl.multiple_of(8 * b, 8)
        lo = jnp.concatenate([prod[o, pl.ds(r, 8), :] for o in range(9)], axis=1)
        hi = jnp.concatenate([prod[o, pl.ds(r + 128, 8), :] for o in range(9)], axis=1)
        fold[pl.ds(r, 8), :] = lo[:, 0:WIDE] + hi[:, 128:128 + WIDE]
        return carry

    lax.fori_loop(0, 16, fold_128, 0)
    for n in (64, 32, 16, 8):
        def fold_n(b, carry, n=n):
            r = pl.multiple_of(8 * b, 8)
            fold[pl.ds(r, 8), :] += pltpu.roll(fold[pl.ds(r + n, 8), :], WIDE - n, 1)
            return carry

        lax.fori_loop(0, n // 8, fold_n, 0)
    v = fold[0:8, :]
    for n in (4, 2, 1):
        v = v + pltpu.roll(pltpu.roll(v, WIDE - n, 1), 8 - n, 0)

    for i in range(NROW):
        vb[i] = v[0:1, 128 * i:128 * (i + 1)]

    def r1_copy(i):
        to = lax.rem(row + i, NROW)
        return pltpu.make_async_remote_copy(
            src_ref=vb.at[to], dst_ref=rs1.at[i], send_sem=r1s.at[i], recv_sem=r1r.at[i],
            device_id=(to, col), device_id_type=MESH)

    for i in range(1, NROW):
        r1_copy(i).start()
    total = vb[row]
    for i in range(1, NROW):
        r1_copy(i).wait_recv()
        total = total + rs1[i]
    sb[...] = total

    def r2_copy(i):
        return pltpu.make_async_remote_copy(
            src_ref=sb, dst_ref=rs2.at[i], send_sem=r2s.at[i], recv_sem=r2r.at[i],
            device_id=(row, lax.rem(col + i, NCOL)), device_id_type=MESH)

    for i in range(1, NCOL):
        r2_copy(i).start()
    for i in range(1, NCOL):
        r2_copy(i).wait_recv()
        total = total + rs2[i]
    total = total * (1.0 / math.sqrt(ROWS * NROW * CB * NCOL))
    total = pltpu.roll(jnp.broadcast_to(total, (8, 128)), lax.rem(128 - 16 * col, 128), 1)
    corr_ref[...] = total

    for side in range(2):
        col_copy(side).wait_send()
        for cp in row_copies(side):
            cp.wait_send()
        halo_tile_copy(side).wait_send()

    def drain(c, carry):
        y_copy(c).wait_send()
        x_copy(c).wait_send()
        w_copy(2 * c).wait()
        w_copy(2 * c + 1).wait()
        return carry

    lax.fori_loop(0, CHUNKS, drain, 0)
    for i in range(1, NROW):
        r1_copy(i).wait_send()
    for i in range(1, NCOL):
        r2_copy(i).wait_send()


def on_device(spins_up, uniforms, moments, accept_bar):
    f32, bf16 = jnp.float32, jnp.bfloat16
    vmem, dma = pltpu.VMEM, pltpu.SemaphoreType.DMA
    hbm = pl.BlockSpec(memory_space=pl.ANY)
    weighted, corr = pl.pallas_call(
        kernel,
        out_shape=(
            jax.ShapeDtypeStruct((ROWS, CB), bf16),
            jax.ShapeDtypeStruct((8, 128), f32),
        ),
        in_specs=[hbm, hbm, hbm, pl.BlockSpec(memory_space=pltpu.SMEM)],
        out_specs=(hbm, pl.BlockSpec(memory_space=pltpu.VMEM)),
        scratch_shapes=[
            vmem((LT, ROWS + 16, 128), jnp.int32),
            vmem((2, LT, ROWS + 16, 128), f32),
            vmem((2, 2, HALO, CB), f32),
            vmem((2, HALO, CB), jnp.int32),
            vmem((ROWS, CB), bf16),
            vmem((3, ROWS + 16, 128), f32),
            vmem((PAIRS + 2, LT + 1, 8, 128), f32),
            vmem((PAIRS + 2, LT + 1, 8, 128), f32),
            vmem((LT, UNIT + 16, 128), f32),
            vmem((ROWS, CB), bf16),
            vmem((CHUNKS, 32, UNIT, TILE), bf16),
            vmem((TILE, 16 * UNIT), bf16),
            vmem((9, TILE, TILE), f32),
            vmem((128, WIDE), f32),
            vmem((2, 16, ROWS), bf16),
            vmem((2, 16, ROWS), bf16),
            vmem((NROW, 1, 128), f32),
            vmem((NROW, 1, 128), f32),
            vmem((NCOL, 1, 128), f32),
            vmem((1, 128), f32),
            dma((4, LT)), dma((4, LT)), dma((10,)), dma((10,)),
            dma((2,)), dma((2,)), dma((6,)), dma((6,)),
            dma((CHUNKS,)), dma((CHUNKS,)), dma((CHUNKS,)), dma((CHUNKS,)),
            dma((NROW,)), dma((NROW,)), dma((NCOL,)), dma((NCOL,)),
        ],
        compiler_params=pltpu.CompilerParams(
            collective_id=0, has_side_effects=True, vmem_limit_bytes=56 * 1024 * 1024,
        ),
    )(spins_up, uniforms, moments, accept_bar)
    lattice = jnp.where(weighted > 0, 1.0, -1.0).astype(f32)
    return lattice, corr[0, :16]


def solution(mesh):
    placed = (P("row", "col"), P(None, "row", "col"), P("row", "col"), P())
    return jax.shard_map(
        on_device,
        mesh=mesh,
        in_specs=placed,
        out_specs=(P("row", "col"), P(("row", "col"))),
        check_vma=False,
    )
```

```python
import math

import jax
import jax.numpy as jnp
from jax import lax
from jax.experimental import pallas as pl
from jax.experimental.pallas import tpu as pltpu
from jax.sharding import PartitionSpec as P

ROWS = 640
CB = 2048
R = 2048
NROW = 16
NCOL = 8
HALO = 8
UNIT = 64
WIDE = CB + 128
TILE = 256
LT = CB // 128
EDGES = (0, LT - 1)
BANDS = ((280, 80), (152, 128), (360, 128), (0, 152), (488, 152), (0, 640))
M_BANDS = ((288, 64), (0, 288), (352, 288))
PARTS = (32, 64, 64, 64, 64, 32)
SPAN = (UNIT + 2 * HALO) // 8
PAIRS = SPAN // 2
MESH = pl.DeviceIdType.MESH


def kernel(
    su_hbm, u_hbm, m_hbm, bar, w_ref, corr_ref,
    su, u, hu, hs, m, ht, c0, c1, wk, small, large, lt, prod, fold, outbox, inbox, vb, rs1, rs2, sb,
    u_sem, s_sem, m_sem, col_send, col_recv,
    row_send, row_recv, ys, yr, xs, xr, r1s, r1r, r2s, r2r,
):
    f32, bf16 = jnp.float32, jnp.bfloat16
    row = lax.axis_index("row")
    col = lax.axis_index("col")
    par = lax.rem(col, 2)
    xcol = col + 1 - 2 * par
    ycol = lax.rem(col + 6 + 4 * par, NCOL)
    left, right = lax.rem(col + NCOL - 1, NCOL), lax.rem(col + 1, NCOL)
    up, down = lax.rem(row + NROW - 1, NROW), lax.rem(row + 1, NROW)
    own = 16 * par
    far = 16 * (1 - par)

    barrier = pltpu.get_barrier_semaphore()
    for i in range(1, NROW):
        pl.semaphore_signal(
            barrier, inc=1, device_id=(lax.rem(row + i, NROW), col), device_id_type=MESH
        )
    for i in range(1, NCOL):
        pl.semaphore_signal(
            barrier, inc=1, device_id=(row, lax.rem(col + i, NCOL)), device_id_type=MESH
        )

    def tile_copies(t, band):
        at, size = BANDS[band]
        lanes = pl.ds(128 * t, 128)
        return (
            pltpu.make_async_copy(
                u_hbm.at[:, pl.ds(at, size), lanes],
                u.at[:, t, pl.ds(at + HALO, size), :], u_sem.at[band, t]),
            pltpu.make_async_copy(
                su_hbm.at[pl.ds(at, size), lanes],
                su.at[t, pl.ds(at + HALO, size), :], s_sem.at[band, t]),
        )

    def m_copy(band):
        rows = pl.ds(*M_BANDS[band])
        return pltpu.make_async_copy(m_hbm.at[rows, :], m.at[rows, :], m_sem.at[band])

    def start_band(band):
        tiles = EDGES if band == 5 else range(1, LT - 1)
        for t in tiles:
            for cp in tile_copies(t, band):
                cp.start()

    def wait_band(band):
        tiles = EDGES if band == 5 else range(1, LT - 1)
        for t in tiles:
            for cp in tile_copies(t, band):
                cp.wait()

    start_band(5)
    start_band(0)
    m_copy(0).start()

    a0 = bar[0]
    a1 = bar[1]

    def limit(draws):
        return jnp.where(draws < a1, 4.0, jnp.where(draws < a0, 2.0, 0.0)).astype(f32)

    def select(side, k):
        r = lax.broadcasted_iota(jnp.int32, (16, 128), 0)
        c = lax.broadcasted_iota(jnp.int32, (16, 128), 1)
        c = c - 124 * side
        hit = (c >= 0) & (c < 4) & (r == 4 * k + c)
        return jnp.where(hit, 1.0, 0.0).astype(bf16)

    wait_band(5)

    for b in range(5):
        r = HALO + 128 * b
        dst = pl.ds(128 * b, 128)
        for side in range(2):
            t = EDGES[side]
            parts = (
                (2 * su[t, pl.ds(r, 128), :] - 1).astype(f32),
                limit(u[0, t, pl.ds(r, 128), :]),
                limit(u[1, t, pl.ds(r, 128), :]),
            )
            msg = jnp.zeros((16, 128), f32)
            for k, x in enumerate(parts):
                msg = msg + lax.dot_general(
                    select(side, k), x.astype(bf16), (((1,), (1,)), ((), ())),
                    preferred_element_type=f32)
            outbox[side, :, dst] = msg.astype(bf16)

    pl.semaphore_wait(barrier, NROW + NCOL - 2)

    def col_copy(side):
        return pltpu.make_async_remote_copy(
            src_ref=outbox.at[side], dst_ref=inbox.at[side],
            send_sem=col_send.at[side], recv_sem=col_recv.at[side],
            device_id=(row, left if side == 0 else right), device_id_type=MESH)

    for side in range(2):
        col_copy(side).start()

    def row_copies(side):
        dev = (down if side == 0 else up, col)
        src_at = ROWS - HALO if side == 0 else 0
        return (
            pltpu.make_async_remote_copy(
                src_ref=u_hbm.at[:, pl.ds(src_at, HALO), :], dst_ref=hu.at[side],
                send_sem=row_send.at[3 * side], recv_sem=row_recv.at[3 * side],
                device_id=dev, device_id_type=MESH),
            pltpu.make_async_remote_copy(
                src_ref=su_hbm.at[pl.ds(src_at, HALO), :], dst_ref=hs.at[side],
                send_sem=row_send.at[3 * side + 1], recv_sem=row_recv.at[3 * side + 1],
                device_id=dev, device_id_type=MESH),
        )

    def halo_tile_copy(side):
        dev = (down if side == 0 else up, col)
        src_at = ROWS if side == 0 else HALO
        dst_at = 0 if side == 0 else ROWS + HALO
        return pltpu.make_async_remote_copy(
            src_ref=ht.at[:, pl.ds(src_at, HALO), :], dst_ref=ht.at[:, pl.ds(dst_at, HALO), :],
            send_sem=row_send.at[3 * side + 2], recv_sem=row_recv.at[3 * side + 2],
            device_id=dev, device_id_type=MESH)

    for side in range(2):
        for cp in row_copies(side):
            cp.start()
    for band in (1, 2):
        start_band(band)
        m_copy(band).start()
    for band in (3, 4):
        start_band(band)

    for side in range(2):
        col_copy(side).wait_recv()

    for b in range(5):
        r = HALO + 128 * b
        src = pl.ds(128 * b, 128)
        for k in range(3):
            tile = jnp.zeros((128, 128), f32)
            for side in range(2):
                tile = tile + lax.dot_general(
                    inbox[side, :, src], select(side, k), (((0,), (0,)), ((), ())),
                    preferred_element_type=f32)
            ht[k, pl.ds(r, 128), :] = tile
    for side in range(2):
        halo_tile_copy(side).start()

    def part(c):
        return small.at[c // 5] if c in (0, 5) else large.at[c - 1]

    def y_copy(c, ref):
        return pltpu.make_async_remote_copy(
            src_ref=ref.at[pl.ds(own, 8)], dst_ref=ref.at[pl.ds(far, 8)],
            send_sem=ys.at[c], recv_sem=yr.at[c],
            device_id=(row, ycol), device_id_type=MESH)

    def x_copy(c, ref):
        return pltpu.make_async_remote_copy(
            src_ref=ref.at[pl.ds(24, 8)], dst_ref=ref.at[pl.ds(8, 8)],
            send_sem=xs.at[c], recv_sem=xr.at[c],
            device_id=(row, xcol), device_id_type=MESH)

    lane = lax.broadcasted_iota(jnp.int32, (8, 128), 1)
    even = lax.rem(lane, 2) == 0
    first, last = lane == 0, lane == 127
    colours = (c0, c1)

    def wrap(ref):
        for t in range(LT + 1):
            ref[0, t] = pltpu.roll(ref[PAIRS, t], 1, 0)
            ref[PAIRS + 1, t] = pltpu.roll(ref[1, t], 7, 0)

    def weigh(c, ref, half, row0, start, count):
        keep = 1 - lax.rem(half + par, 2)
        base = own * keep + 24 * (1 - keep)
        for g in range(count // 16):
            at = pl.multiple_of(row0 + start + 16 * g, 16)
            for t in range(LT):
                lanes = pl.ds(128 * t, 128)
                w = m[pl.ds(at, 16), lanes] * wk[t, HALO + start + 16 * g:HALO + start + 16 * g + 16, :].astype(bf16)
                ref[base + t // 2, 16 * g:16 * g + 16, 128 * (t % 2):128 * (t % 2 + 1)] = w
                w_ref[pl.ds(at, 16), lanes] = w

        @pl.when(keep == 1)
        def _():
            y_copy(c, ref).start()

        @pl.when(keep == 0)
        def _():
            x_copy(c, ref).start()

    def unit(k, carry):
        i = lax.div(k + 1, 2)
        odd = lax.rem(k, 2)
        row0 = jnp.minimum(jnp.maximum(288 + UNIT * i * (1 - 2 * odd), 0), ROWS - UNIT)

        for n in range(4):
            @pl.when(k == 1 + n)
            def _():
                wait_band(1 + n)
                if n < 2:
                    m_copy(1 + n).wait()

        for side in range(2):
            @pl.when(k == 9 + side)
            def _():
                for cp in row_copies(side):
                    cp.wait_recv()
                halo_tile_copy(side).wait_recv()
                at = 0 if side == 0 else ROWS + HALO
                for t in range(LT):
                    lanes = pl.ds(128 * t, 128)
                    su[t, at:at + HALO, :] = hs[side, :, lanes]
                    for n in range(2):
                        u[n, t, at:at + HALO, :] = hu[side, n, :, lanes]

        for g in range(PAIRS):
            upper = pl.ds(row0 + 2 * g, 8, stride=SPAN)
            lower = pl.ds(row0 + 2 * g + 1, 8, stride=SPAN)
            for t in range(LT + 1):
                if t < LT:
                    a = (2 * su[t, upper, :] - 1).astype(f32)
                    b = (2 * su[t, lower, :] - 1).astype(f32)
                else:
                    a, b = ht[0, upper, :], ht[0, lower, :]
                c0[g + 1, t] = jnp.where(even, a, b)
                c1[g + 1, t] = jnp.where(even, b, a)
        wrap(c1)

        for h in range(4):
            sweep, colour = h // 2, h % 2
            mine, other = colours[colour], colours[1 - colour]

            for g in range(PAIRS):
                upper = pl.ds(row0 + 2 * g + colour, 8, stride=SPAN)
                lower = pl.ds(row0 + 2 * g + 1 - colour, 8, stride=SPAN)
                mid = [other[g + 1, t] for t in range(LT + 1)]
                east = [pltpu.roll(x, 1, 1) for x in mid]
                west = [pltpu.roll(x, 127, 1) for x in mid]
                for t in range(LT + 1):
                    above, below = other[g, t], other[g + 2, t]
                    outer = jnp.where(even, above, below) if colour == 0 else jnp.where(even, below, above)
                    side = (jnp.where(first, east[t - 1], east[t])
                            + jnp.where(last, west[(t + 1) % (LT + 1)], west[t]))
                    if t < LT:
                        bound = limit(jnp.where(even, u[sweep, t, upper, :], u[sweep, t, lower, :]))
                    else:
                        bound = jnp.where(even, ht[1 + sweep, upper, :], ht[1 + sweep, lower, :])
                    cur = mine[g + 1, t]
                    flip = cur * (mid[t] + outer + side) <= bound
                    mine[g + 1, t] = jnp.where(flip, -cur, cur)
            if h < 3:
                wrap(mine)

        for g in range(PAIRS):
            for t in range(LT):
                a, b = c0[g + 1, t], c1[g + 1, t]
                wk[t, pl.ds(2 * g, 8, stride=SPAN), :] = jnp.where(even, a, b)
                wk[t, pl.ds(2 * g + 1, 8, stride=SPAN), :] = jnp.where(even, b, a)

        @pl.when(k == 0)
        def _():
            for half in range(2):
                weigh(0, small.at[0], half, row0, 32 * half, 32)

        @pl.when((k > 0) & (k < 9))
        def _():
            weigh(i, large.at[i - 1], 1 - odd, row0, 0, UNIT)

        for half in range(2):
            @pl.when(k == 9 + half)
            def _():
                weigh(5, small.at[1], half, row0, 32 * half, 32)

        return carry

    wait_band(0)
    m_copy(0).wait()
    lax.fori_loop(0, 11, unit, 0)

    def chunk(c, ref, height, opening):
        y_copy(c, ref).wait_recv()
        x_copy(c, ref).wait_recv()
        depth = 16 * height
        per = 128 // height
        for n in range(depth // 128):
            rows = ref[per * n:per * n + per].reshape(128, TILE)
            lt[:, 128 * n:128 * (n + 1)] = rows.T
        for o in range(9):
            right = ref[o:o + 16].reshape(depth, TILE)
            p = jnp.dot(lt[:, 0:depth], right, preferred_element_type=f32)
            prod[o] = p if opening else prod[o] + p

    chunk(0, small.at[0], 32, True)

    def middle(c, carry):
        chunk(c + 1, large.at[c], UNIT, False)
        return carry

    lax.fori_loop(0, 4, middle, 0)
    chunk(5, small.at[1], 32, False)

    for b in range(16):
        r = 8 * b
        lo = jnp.concatenate([prod[o, pl.ds(r, 8), :] for o in range(9)], axis=1)
        hi = jnp.concatenate([prod[o, pl.ds(r + 128, 8), :] for o in range(9)], axis=1)
        fold[pl.ds(r, 8), :] = lo[:, 0:WIDE] + hi[:, 128:128 + WIDE]
    for n in (64, 32, 16, 8):
        for b in range(n // 8):
            r = 8 * b
            fold[pl.ds(r, 8), :] += pltpu.roll(fold[pl.ds(r + n, 8), :], WIDE - n, 1)
    v = fold[0:8, :]
    for n in (4, 2, 1):
        v = v + pltpu.roll(pltpu.roll(v, WIDE - n, 1), 8 - n, 0)

    for i in range(NROW):
        vb[i] = v[0:1, 128 * i:128 * (i + 1)]

    def r1_copy(i):
        to = lax.rem(row + i, NROW)
        return pltpu.make_async_remote_copy(
            src_ref=vb.at[to], dst_ref=rs1.at[i], send_sem=r1s.at[i], recv_sem=r1r.at[i],
            device_id=(to, col), device_id_type=MESH)

    for i in range(1, NROW):
        r1_copy(i).start()
    total = vb[row]
    for i in range(1, NROW):
        r1_copy(i).wait_recv()
        total = total + rs1[i]
    sb[...] = total

    def r2_copy(i):
        return pltpu.make_async_remote_copy(
            src_ref=sb, dst_ref=rs2.at[i], send_sem=r2s.at[i], recv_sem=r2r.at[i],
            device_id=(row, lax.rem(col + i, NCOL)), device_id_type=MESH)

    for i in range(1, NCOL):
        r2_copy(i).start()
    for i in range(1, NCOL):
        r2_copy(i).wait_recv()
        total = total + rs2[i]
    total = total * (1.0 / math.sqrt(ROWS * NROW * CB * NCOL))
    total = pltpu.roll(jnp.broadcast_to(total, (8, 128)), lax.rem(128 - 16 * col, 128), 1)
    corr_ref[...] = total

    for side in range(2):
        col_copy(side).wait_send()
        for cp in row_copies(side):
            cp.wait_send()
        halo_tile_copy(side).wait_send()

    for c in range(len(PARTS)):
        y_copy(c, part(c)).wait_send()
        x_copy(c, part(c)).wait_send()
    for i in range(1, NROW):
        r1_copy(i).wait_send()
    for i in range(1, NCOL):
        r2_copy(i).wait_send()


def finish(w_ref, reduced_ref, spins_ref, corr_ref):
    spins_ref[...] = jnp.where(w_ref[...].astype(jnp.float32) > 0, 1.0, -1.0)
    corr_ref[...] = reduced_ref[0, :16]


def on_device(spins_up, uniforms, moments, accept_bar):
    f32, bf16 = jnp.float32, jnp.bfloat16
    vmem, dma = pltpu.VMEM, pltpu.SemaphoreType.DMA
    hbm = pl.BlockSpec(memory_space=pl.ANY)
    weighted, corr = pl.pallas_call(
        kernel,
        out_shape=(
            jax.ShapeDtypeStruct((ROWS, CB), bf16),
            jax.ShapeDtypeStruct((8, 128), f32),
        ),
        in_specs=[hbm, hbm, hbm, pl.BlockSpec(memory_space=pltpu.SMEM)],
        out_specs=(pl.BlockSpec(memory_space=pltpu.VMEM), pl.BlockSpec(memory_space=pltpu.VMEM)),
        scratch_shapes=[
            vmem((LT, ROWS + 16, 128), jnp.int32),
            vmem((2, LT, ROWS + 16, 128), f32),
            vmem((2, 2, HALO, CB), f32),
            vmem((2, HALO, CB), jnp.int32),
            vmem((ROWS, CB), bf16),
            vmem((3, ROWS + 16, 128), f32),
            vmem((PAIRS + 2, LT + 1, 8, 128), f32),
            vmem((PAIRS + 2, LT + 1, 8, 128), f32),
            vmem((LT, UNIT + 16, 128), f32),
            vmem((2, 32, 32, TILE), bf16),
            vmem((4, 32, UNIT, TILE), bf16),
            vmem((TILE, 16 * UNIT), bf16),
            vmem((9, TILE, TILE), f32),
            vmem((128, WIDE), f32),
            vmem((2, 16, ROWS), bf16),
            vmem((2, 16, ROWS), bf16),
            vmem((NROW, 1, 128), f32),
            vmem((NROW, 1, 128), f32),
            vmem((NCOL, 1, 128), f32),
            vmem((1, 128), f32),
            dma((len(BANDS), LT)), dma((len(BANDS), LT)), dma((3,)),
            dma((2,)), dma((2,)), dma((6,)), dma((6,)),
            dma((len(PARTS),)), dma((len(PARTS),)), dma((len(PARTS),)), dma((len(PARTS),)),
            dma((NROW,)), dma((NROW,)), dma((NCOL,)), dma((NCOL,)),
        ],
        compiler_params=pltpu.CompilerParams(
            collective_id=0, has_side_effects=True, vmem_limit_bytes=56 * 1024 * 1024,
        ),
    )(spins_up, uniforms, moments, accept_bar)
    block = 128
    return pl.pallas_call(
        finish,
        grid=(ROWS // block,),
        out_shape=(
            jax.ShapeDtypeStruct((ROWS, CB), f32),
            jax.ShapeDtypeStruct((16,), f32),
        ),
        in_specs=[
            pl.BlockSpec((block, CB), lambda i: (i, 0)),
            pl.BlockSpec((8, 128), lambda i: (0, 0)),
        ],
        out_specs=(
            pl.BlockSpec((block, CB), lambda i: (i, 0)),
            pl.BlockSpec((16,), lambda i: (0,)),
        ),
    )(weighted, corr)


def solution(mesh):
    placed = (P("row", "col"), P(None, "row", "col"), P("row", "col"), P())
    return jax.shard_map(
        on_device,
        mesh=mesh,
        in_specs=placed,
        out_specs=(P("row", "col"), P(("row", "col"))),
        check_vma=False,
    )
```

```python
import math

import jax
import jax.numpy as jnp
from jax import lax
from jax.experimental import pallas as pl
from jax.experimental.pallas import tpu as pltpu
from jax.sharding import PartitionSpec as P

ROWS = 640
CB = 2048
R = 2048
NROW = 16
NCOL = 8
HALO = 8
UNIT = 64
WIDE = CB + 128
TILE = 256
LT = CB // 128
EDGES = (0, LT - 1)
BANDS = ((248, 144), (56, 192), (392, 192), (0, 56), (584, 56), (0, 640))
M_BANDS = ((256, 128), (0, 256), (384, 256))
SENDS = ((0, 1, 6), (0, 0, 1), (0, 7, 1), (1, 0, 8), (2, 0, 8), (3, 0, 8), (4, 0, 8), (5, 0, 8))
SPAN = (UNIT + 2 * HALO) // 8
PAIRS = SPAN // 2
MESH = pl.DeviceIdType.MESH


def kernel(
    su_hbm, u_hbm, m_hbm, bar, w_ref, corr_ref,
    su, u, hu, hs, m, ht, c0, c1, wk, small, large, lt, prod, fold, outbox, inbox, vb, rs1, rs2, sb,
    u_sem, s_sem, m_sem, col_send, col_recv,
    row_send, row_recv, ys, yr, xs, xr, r1s, r1r, r2s, r2r,
):
    f32, bf16 = jnp.float32, jnp.bfloat16
    row = lax.axis_index("row")
    col = lax.axis_index("col")
    par = lax.rem(col, 2)
    xcol = col + 1 - 2 * par
    ycol = lax.rem(col + 6 + 4 * par, NCOL)
    left, right = lax.rem(col + NCOL - 1, NCOL), lax.rem(col + 1, NCOL)
    up, down = lax.rem(row + NROW - 1, NROW), lax.rem(row + 1, NROW)
    own = 16 * par
    far = 16 * (1 - par)

    barrier = pltpu.get_barrier_semaphore()
    for i in range(1, NROW):
        pl.semaphore_signal(
            barrier, inc=1, device_id=(lax.rem(row + i, NROW), col), device_id_type=MESH
        )
    for i in range(1, NCOL):
        pl.semaphore_signal(
            barrier, inc=1, device_id=(row, lax.rem(col + i, NCOL)), device_id_type=MESH
        )

    def tile_copies(t, band):
        at, size = BANDS[band]
        lanes = pl.ds(128 * t, 128)
        return (
            pltpu.make_async_copy(
                u_hbm.at[:, pl.ds(at, size), lanes],
                u.at[:, t, pl.ds(at + HALO, size), :], u_sem.at[band, t]),
            pltpu.make_async_copy(
                su_hbm.at[pl.ds(at, size), lanes],
                su.at[t, pl.ds(at + HALO, size), :], s_sem.at[band, t]),
        )

    def m_copy(band):
        rows = pl.ds(*M_BANDS[band])
        return pltpu.make_async_copy(m_hbm.at[rows, :], m.at[rows, :], m_sem.at[band])

    def start_band(band):
        tiles = EDGES if band == 5 else range(1, LT - 1)
        for t in tiles:
            for cp in tile_copies(t, band):
                cp.start()

    def wait_band(band):
        tiles = EDGES if band == 5 else range(1, LT - 1)
        for t in tiles:
            for cp in tile_copies(t, band):
                cp.wait()

    start_band(5)
    start_band(0)
    m_copy(0).start()

    a0 = bar[0]
    a1 = bar[1]

    def limit(draws):
        return jnp.where(draws < a1, 4.0, jnp.where(draws < a0, 2.0, 0.0)).astype(f32)

    def select(side, k):
        r = lax.broadcasted_iota(jnp.int32, (16, 128), 0)
        c = lax.broadcasted_iota(jnp.int32, (16, 128), 1)
        c = c - 124 * side
        hit = (c >= 0) & (c < 4) & (r == 4 * k + c)
        return jnp.where(hit, 1.0, 0.0).astype(bf16)

    for n in range(3):
        for b in range(5):
            ht[n, HALO + 128 * b:HALO + 128 * (b + 1), :] = jnp.zeros((128, 128), f32)
    wait_band(5)

    for b in range(5):
        r = HALO + 128 * b
        dst = pl.ds(128 * b, 128)
        for side in range(2):
            t = EDGES[side]
            parts = (
                (2 * su[t, pl.ds(r, 128), :] - 1).astype(f32),
                limit(u[0, t, pl.ds(r, 128), :]),
                limit(u[1, t, pl.ds(r, 128), :]),
            )
            msg = jnp.zeros((16, 128), f32)
            for k, x in enumerate(parts):
                msg = msg + lax.dot_general(
                    select(side, k), x.astype(bf16), (((1,), (1,)), ((), ())),
                    preferred_element_type=f32)
            outbox[side, :, dst] = msg.astype(bf16)

    pl.semaphore_wait(barrier, NROW + NCOL - 2)

    def col_copy(side):
        return pltpu.make_async_remote_copy(
            src_ref=outbox.at[side], dst_ref=inbox.at[side],
            send_sem=col_send.at[side], recv_sem=col_recv.at[side],
            device_id=(row, left if side == 0 else right), device_id_type=MESH)

    for side in range(2):
        col_copy(side).start()

    def row_copies(side):
        dev = (down if side == 0 else up, col)
        src_at = ROWS - HALO if side == 0 else 0
        return (
            pltpu.make_async_remote_copy(
                src_ref=u_hbm.at[:, pl.ds(src_at, HALO), :], dst_ref=hu.at[side],
                send_sem=row_send.at[3 * side], recv_sem=row_recv.at[3 * side],
                device_id=dev, device_id_type=MESH),
            pltpu.make_async_remote_copy(
                src_ref=su_hbm.at[pl.ds(src_at, HALO), :], dst_ref=hs.at[side],
                send_sem=row_send.at[3 * side + 1], recv_sem=row_recv.at[3 * side + 1],
                device_id=dev, device_id_type=MESH),
        )

    def halo_tile_copy(side):
        dev = (down if side == 0 else up, col)
        src_at = ROWS if side == 0 else HALO
        dst_at = 0 if side == 0 else ROWS + HALO
        return pltpu.make_async_remote_copy(
            src_ref=ht.at[:, pl.ds(src_at, HALO), :], dst_ref=ht.at[:, pl.ds(dst_at, HALO), :],
            send_sem=row_send.at[3 * side + 2], recv_sem=row_recv.at[3 * side + 2],
            device_id=dev, device_id_type=MESH)

    for side in range(2):
        for cp in row_copies(side):
            cp.start()
    for band in (1, 2):
        start_band(band)
        m_copy(band).start()
    for band in (3, 4):
        start_band(band)

    def column_halos():
        for side in range(2):
            col_copy(side).wait_recv()

        for b in range(5):
            r = HALO + 128 * b
            src = pl.ds(128 * b, 128)
            for k in range(3):
                tile = jnp.zeros((128, 128), f32)
                for side in range(2):
                    tile = tile + lax.dot_general(
                        inbox[side, :, src], select(side, k), (((0,), (0,)), ((), ())),
                        preferred_element_type=f32)
                ht[k, pl.ds(r, 128), :] = tile
        for side in range(2):
            halo_tile_copy(side).start()

    def part(c):
        return small.at[c - 4] if c >= 4 else large.at[c]

    def y_copy(n, ref):
        _, at, size = SENDS[n]
        return pltpu.make_async_remote_copy(
            src_ref=ref.at[pl.ds(own + at, size)], dst_ref=ref.at[pl.ds(far + at, size)],
            send_sem=ys.at[n], recv_sem=yr.at[n],
            device_id=(row, ycol), device_id_type=MESH)

    def x_copy(n, ref):
        _, at, size = SENDS[n]
        return pltpu.make_async_remote_copy(
            src_ref=ref.at[pl.ds(24 + at, size)], dst_ref=ref.at[pl.ds(8 + at, size)],
            send_sem=xs.at[n], recv_sem=xr.at[n],
            device_id=(row, xcol), device_id_type=MESH)

    def send(keep, n):
        @pl.when(keep == 1)
        def _():
            y_copy(n, part(SENDS[n][0])).start()

        @pl.when(keep == 0)
        def _():
            x_copy(n, part(SENDS[n][0])).start()

    lane = lax.broadcasted_iota(jnp.int32, (8, 128), 1)
    even = lax.rem(lane, 2) == 0
    first, last = lane == 0, lane == 127
    colours = (c0, c1)

    def wrap(ref):
        for t in range(LT + 1):
            ref[0, t] = pltpu.roll(ref[PAIRS, t], 1, 0)
            ref[PAIRS + 1, t] = pltpu.roll(ref[1, t], 7, 0)

    def weigh(ref, keep, row0, start, count, tiles):
        base = own * keep + 24 * (1 - keep)
        for g in range(count // 16):
            at = pl.multiple_of(row0 + start + 16 * g, 16)
            for t in tiles:
                lanes = pl.ds(128 * t, 128)
                w = m[pl.ds(at, 16), lanes] * wk[t, HALO + start + 16 * g:HALO + start + 16 * g + 16, :].astype(bf16)
                ref[base + t // 2, 16 * g:16 * g + 16, 128 * (t % 2):128 * (t % 2 + 1)] = w
                w_ref[pl.ds(at, 16), lanes] = w

    def unit(k, carry):
        p = jnp.maximum(k - 2, lax.rem(k, 2))
        half = lax.rem(p, 2)
        i = lax.div(p, 2)
        keep = 1 - lax.rem(half + par, 2)
        row0 = (256 - UNIT * i) * (1 - half) + (320 + UNIT * i) * half

        @pl.when(k == 2)
        def _():
            column_halos()

        for n in range(2):
            @pl.when(k == 4 + n)
            def _():
                wait_band(1 + n)
                m_copy(1 + n).wait()

            @pl.when(k == 8 + n)
            def _():
                wait_band(3 + n)

        for side in range(2):
            @pl.when(k == 10 + side)
            def _():
                for cp in row_copies(side):
                    cp.wait_recv()
                halo_tile_copy(side).wait_recv()
                at = 0 if side == 0 else ROWS + HALO
                for t in range(LT):
                    lanes = pl.ds(128 * t, 128)
                    su[t, at:at + HALO, :] = hs[side, :, lanes]
                    for n in range(2):
                        u[n, t, at:at + HALO, :] = hu[side, n, :, lanes]

        for g in range(PAIRS):
            upper = pl.ds(row0 + 2 * g, 8, stride=SPAN)
            lower = pl.ds(row0 + 2 * g + 1, 8, stride=SPAN)
            for t in range(LT + 1):
                if t < LT:
                    a = (2 * su[t, upper, :] - 1).astype(f32)
                    b = (2 * su[t, lower, :] - 1).astype(f32)
                else:
                    a, b = ht[0, upper, :], ht[0, lower, :]
                c0[g + 1, t] = jnp.where(even, a, b)
                c1[g + 1, t] = jnp.where(even, b, a)
        wrap(c1)

        for h in range(4):
            sweep, colour = h // 2, h % 2
            mine, other = colours[colour], colours[1 - colour]

            for g in range(PAIRS):
                upper = pl.ds(row0 + 2 * g + colour, 8, stride=SPAN)
                lower = pl.ds(row0 + 2 * g + 1 - colour, 8, stride=SPAN)
                mid = [other[g + 1, t] for t in range(LT + 1)]
                east = [pltpu.roll(x, 1, 1) for x in mid]
                west = [pltpu.roll(x, 127, 1) for x in mid]
                for t in range(LT + 1):
                    above, below = other[g, t], other[g + 2, t]
                    outer = jnp.where(even, above, below) if colour == 0 else jnp.where(even, below, above)
                    side = (jnp.where(first, east[t - 1], east[t])
                            + jnp.where(last, west[(t + 1) % (LT + 1)], west[t]))
                    if t < LT:
                        bound = limit(jnp.where(even, u[sweep, t, upper, :], u[sweep, t, lower, :]))
                    else:
                        bound = jnp.where(even, ht[1 + sweep, upper, :], ht[1 + sweep, lower, :])
                    cur = mine[g + 1, t]
                    flip = cur * (mid[t] + outer + side) <= bound
                    mine[g + 1, t] = jnp.where(flip, -cur, cur)
            if h < 3:
                wrap(mine)

        for g in range(PAIRS):
            for t in range(LT):
                a, b = c0[g + 1, t], c1[g + 1, t]
                wk[t, pl.ds(2 * g, 8, stride=SPAN), :] = jnp.where(even, a, b)
                wk[t, pl.ds(2 * g + 1, 8, stride=SPAN), :] = jnp.where(even, b, a)

        @pl.when(k < 2)
        def _():
            weigh(large.at[0], keep, row0, 0, UNIT, range(2, LT - 2))
            send(keep, 0)

        @pl.when((k >= 2) & (k < 4))
        def _():
            weigh(large.at[0], keep, row0, 0, UNIT, (0, 1, LT - 2, LT - 1))
            send(keep, 1)
            send(keep, 2)

        for c in range(1, 4):
            @pl.when((k >= 2 + 2 * c) & (k < 4 + 2 * c))
            def _():
                weigh(large.at[c], keep, row0, 0, UNIT, range(LT))
                send(keep, 2 + c)

        for side in range(2):
            @pl.when(k == 10 + side)
            def _():
                for n in range(2):
                    weigh(small.at[n], keep, row0, 32 * (1 - n if side == 0 else n), 32, range(LT))
                    send(keep, 6 + n)

        return carry

    wait_band(0)
    m_copy(0).wait()
    lax.fori_loop(0, 12, unit, 0)

    def chunk(c, height, opening):
        ref = part(c)
        for n, what in enumerate(SENDS):
            if what[0] == c:
                y_copy(n, ref).wait_recv()
                x_copy(n, ref).wait_recv()
        depth = 16 * height
        per = 128 // height
        for n in range(depth // 128):
            rows = ref[per * n:per * n + per].reshape(128, TILE)
            lt[:, 128 * n:128 * (n + 1)] = rows.T
        for o in range(9):
            right = ref[o:o + 16].reshape(depth, TILE)
            p = jnp.dot(lt[:, 0:depth], right, preferred_element_type=f32)
            prod[o] = p if opening else prod[o] + p

    for c in range(6):
        chunk(c, UNIT if c < 4 else 32, c == 0)

    for b in range(16):
        r = 8 * b
        lo = jnp.concatenate([prod[o, pl.ds(r, 8), :] for o in range(9)], axis=1)
        hi = jnp.concatenate([prod[o, pl.ds(r + 128, 8), :] for o in range(9)], axis=1)
        fold[pl.ds(r, 8), :] = lo[:, 0:WIDE] + hi[:, 128:128 + WIDE]
    for n in (64, 32, 16, 8):
        for b in range(n // 8):
            r = 8 * b
            fold[pl.ds(r, 8), :] += pltpu.roll(fold[pl.ds(r + n, 8), :], WIDE - n, 1)
    v = fold[0:8, :]
    for n in (4, 2, 1):
        v = v + pltpu.roll(pltpu.roll(v, WIDE - n, 1), 8 - n, 0)

    for i in range(NROW):
        vb[i] = v[0:1, 128 * i:128 * (i + 1)]

    def r1_copy(i):
        to = lax.rem(row + i, NROW)
        return pltpu.make_async_remote_copy(
            src_ref=vb.at[to], dst_ref=rs1.at[i], send_sem=r1s.at[i], recv_sem=r1r.at[i],
            device_id=(to, col), device_id_type=MESH)

    for i in range(1, NROW):
        r1_copy(i).start()
    total = vb[row]
    for i in range(1, NROW):
        r1_copy(i).wait_recv()
        total = total + rs1[i]
    sb[...] = total

    def r2_copy(i):
        return pltpu.make_async_remote_copy(
            src_ref=sb, dst_ref=rs2.at[i], send_sem=r2s.at[i], recv_sem=r2r.at[i],
            device_id=(row, lax.rem(col + i, NCOL)), device_id_type=MESH)

    for i in range(1, NCOL):
        r2_copy(i).start()
    for i in range(1, NCOL):
        r2_copy(i).wait_recv()
        total = total + rs2[i]
    total = total * (1.0 / math.sqrt(ROWS * NROW * CB * NCOL))
    total = pltpu.roll(jnp.broadcast_to(total, (8, 128)), lax.rem(128 - 16 * col, 128), 1)
    corr_ref[...] = total

    for side in range(2):
        col_copy(side).wait_send()
        for cp in row_copies(side):
            cp.wait_send()
        halo_tile_copy(side).wait_send()

    for n, what in enumerate(SENDS):
        y_copy(n, part(what[0])).wait_send()
        x_copy(n, part(what[0])).wait_send()
    for i in range(1, NROW):
        r1_copy(i).wait_send()
    for i in range(1, NCOL):
        r2_copy(i).wait_send()


def finish(w_ref, reduced_ref, spins_hbm, corr_ref, spins, sem):
    block = 64
    copies = []
    for i in range(ROWS // block):
        rows = pl.ds(block * i, block)
        spins[rows, :] = jnp.where(w_ref[rows, :].astype(jnp.float32) > 0, 1.0, -1.0)
        copies.append(pltpu.make_async_copy(spins.at[rows, :], spins_hbm.at[rows, :], sem.at[i]))
        copies[-1].start()
    corr_ref[...] = reduced_ref[0, :16]
    for cp in copies:
        cp.wait()


def on_device(spins_up, uniforms, moments, accept_bar):
    f32, bf16 = jnp.float32, jnp.bfloat16
    vmem, dma = pltpu.VMEM, pltpu.SemaphoreType.DMA
    hbm = pl.BlockSpec(memory_space=pltpu.HBM)
    weighted, corr = pl.pallas_call(
        kernel,
        out_shape=(
            jax.ShapeDtypeStruct((ROWS, CB), bf16),
            jax.ShapeDtypeStruct((8, 128), f32),
        ),
        in_specs=[hbm, hbm, hbm, pl.BlockSpec(memory_space=pltpu.SMEM)],
        out_specs=(pl.BlockSpec(memory_space=pltpu.VMEM), pl.BlockSpec(memory_space=pltpu.VMEM)),
        scratch_shapes=[
            vmem((LT, ROWS + 16, 128), jnp.int32),
            vmem((2, LT, ROWS + 16, 128), f32),
            vmem((2, 2, HALO, CB), f32),
            vmem((2, HALO, CB), jnp.int32),
            vmem((ROWS, CB), bf16),
            vmem((3, ROWS + 16, 128), f32),
            vmem((PAIRS + 2, LT + 1, 8, 128), f32),
            vmem((PAIRS + 2, LT + 1, 8, 128), f32),
            vmem((LT, UNIT + 16, 128), f32),
            vmem((2, 32, 32, TILE), bf16),
            vmem((4, 32, UNIT, TILE), bf16),
            vmem((TILE, 16 * UNIT), bf16),
            vmem((9, TILE, TILE), f32),
            vmem((128, WIDE), f32),
            vmem((2, 16, ROWS), bf16),
            vmem((2, 16, ROWS), bf16),
            vmem((NROW, 1, 128), f32),
            vmem((NROW, 1, 128), f32),
            vmem((NCOL, 1, 128), f32),
            vmem((1, 128), f32),
            dma((len(BANDS), LT)), dma((len(BANDS), LT)), dma((3,)),
            dma((2,)), dma((2,)), dma((6,)), dma((6,)),
            dma((len(SENDS),)), dma((len(SENDS),)), dma((len(SENDS),)), dma((len(SENDS),)),
            dma((NROW,)), dma((NROW,)), dma((NCOL,)), dma((NCOL,)),
        ],
        compiler_params=pltpu.CompilerParams(
            collective_id=0, has_side_effects=True, vmem_limit_bytes=50 * 1024 * 1024,
        ),
    )(spins_up, uniforms, moments, accept_bar)
    in_vmem = pl.BlockSpec(memory_space=pltpu.VMEM)
    return pl.pallas_call(
        finish,
        out_shape=(
            jax.ShapeDtypeStruct((ROWS, CB), f32),
            jax.ShapeDtypeStruct((16,), f32),
        ),
        in_specs=[in_vmem, in_vmem],
        out_specs=(hbm, in_vmem),
        scratch_shapes=[vmem((ROWS, CB), f32), dma((10,))],
        compiler_params=pltpu.CompilerParams(vmem_limit_bytes=16 * 1024 * 1024),
    )(weighted, corr)


def solution(mesh):
    placed = (P("row", "col"), P(None, "row", "col"), P("row", "col"), P())
    return jax.shard_map(
        on_device,
        mesh=mesh,
        in_specs=placed,
        out_specs=(P("row", "col"), P(("row", "col"))),
        check_vma=False,
    )
```

```python
import math

import jax
import jax.numpy as jnp
from jax import lax
from jax.experimental import pallas as pl
from jax.experimental.pallas import tpu as pltpu
from jax.sharding import PartitionSpec as P

ROWS = 640
CB = 2048
R = 2048
NROW = 16
NCOL = 8
HALO = 8
UNIT = 64
WIDE = CB + 128
TILE = 256
LT = CB // 128
EDGES = (0, LT - 1)
BANDS = ((216, 208), (88, 128), (424, 128), (0, 88), (552, 88), (0, 640))
M_BANDS = ((224, 192), (0, 224), (416, 224))
SENDS = (
    (0, 1, 6), (1, 1, 6), (0, 0, 1), (0, 7, 1), (1, 0, 1), (1, 7, 1),
    (2, 0, 8), (3, 0, 8), (4, 0, 8), (5, 0, 8), (6, 0, 8),
)
HEIGHTS = (32, 64, 64, 64, 64, 16, 16)
SPAN = (UNIT + 2 * HALO) // 8
PAIRS = SPAN // 2
MESH = pl.DeviceIdType.MESH


def kernel(
    su_hbm, u_hbm, m_hbm, bar, w_ref, corr_ref,
    su, u, hu, hs, m, ht, c0, c1, wk, small, large, tiny, lt, prod, fold, outbox, inbox, vb, rs1, rs2, sb,
    u_sem, s_sem, m_sem, col_send, col_recv,
    row_send, row_recv, ys, yr, xs, xr, r1s, r1r, r2s, r2r,
):
    f32, bf16 = jnp.float32, jnp.bfloat16
    row = lax.axis_index("row")
    col = lax.axis_index("col")
    par = lax.rem(col, 2)
    xcol = col + 1 - 2 * par
    ycol = lax.rem(col + 6 + 4 * par, NCOL)
    left, right = lax.rem(col + NCOL - 1, NCOL), lax.rem(col + 1, NCOL)
    up, down = lax.rem(row + NROW - 1, NROW), lax.rem(row + 1, NROW)
    own = 16 * par
    far = 16 * (1 - par)

    barrier = pltpu.get_barrier_semaphore()
    for i in range(1, NROW):
        pl.semaphore_signal(
            barrier, inc=1, device_id=(lax.rem(row + i, NROW), col), device_id_type=MESH
        )
    for i in range(1, NCOL):
        pl.semaphore_signal(
            barrier, inc=1, device_id=(row, lax.rem(col + i, NCOL)), device_id_type=MESH
        )

    def tile_copies(t, band):
        at, size = BANDS[band]
        lanes = pl.ds(128 * t, 128)
        return (
            pltpu.make_async_copy(
                u_hbm.at[:, pl.ds(at, size), lanes],
                u.at[:, t, pl.ds(at + HALO, size), :], u_sem.at[band, t]),
            pltpu.make_async_copy(
                su_hbm.at[pl.ds(at, size), lanes],
                su.at[t, pl.ds(at + HALO, size), :], s_sem.at[band, t]),
        )

    def m_copy(band):
        rows = pl.ds(*M_BANDS[band])
        return pltpu.make_async_copy(m_hbm.at[rows, :], m.at[rows, :], m_sem.at[band])

    def start_band(band):
        tiles = EDGES if band == 5 else range(1, LT - 1)
        for t in tiles:
            for cp in tile_copies(t, band):
                cp.start()

    def wait_band(band):
        tiles = EDGES if band == 5 else range(1, LT - 1)
        for t in tiles:
            for cp in tile_copies(t, band):
                cp.wait()

    start_band(5)
    start_band(0)
    m_copy(0).start()

    a0 = bar[0]
    a1 = bar[1]

    def limit(draws):
        return jnp.where(draws < a1, 4.0, jnp.where(draws < a0, 2.0, 0.0)).astype(f32)

    def select(side, k):
        r = lax.broadcasted_iota(jnp.int32, (16, 128), 0)
        c = lax.broadcasted_iota(jnp.int32, (16, 128), 1)
        c = c - 124 * side
        hit = (c >= 0) & (c < 4) & (r == 4 * k + c)
        return jnp.where(hit, 1.0, 0.0).astype(bf16)

    for n in range(3):
        for b in range(5):
            ht[n, HALO + 128 * b:HALO + 128 * (b + 1), :] = jnp.zeros((128, 128), f32)
    wait_band(5)

    for b in range(5):
        r = HALO + 128 * b
        dst = pl.ds(128 * b, 128)
        for side in range(2):
            t = EDGES[side]
            parts = (
                (2 * su[t, pl.ds(r, 128), :] - 1).astype(f32),
                limit(u[0, t, pl.ds(r, 128), :]),
                limit(u[1, t, pl.ds(r, 128), :]),
            )
            msg = jnp.zeros((16, 128), f32)
            for k, x in enumerate(parts):
                msg = msg + lax.dot_general(
                    select(side, k), x.astype(bf16), (((1,), (1,)), ((), ())),
                    preferred_element_type=f32)
            outbox[side, :, dst] = msg.astype(bf16)

    pl.semaphore_wait(barrier, NROW + NCOL - 2)

    def col_copy(side):
        return pltpu.make_async_remote_copy(
            src_ref=outbox.at[side], dst_ref=inbox.at[side],
            send_sem=col_send.at[side], recv_sem=col_recv.at[side],
            device_id=(row, left if side == 0 else right), device_id_type=MESH)

    for side in range(2):
        col_copy(side).start()

    def row_copies(side):
        dev = (down if side == 0 else up, col)
        src_at = ROWS - HALO if side == 0 else 0
        return (
            pltpu.make_async_remote_copy(
                src_ref=u_hbm.at[:, pl.ds(src_at, HALO), :], dst_ref=hu.at[side],
                send_sem=row_send.at[3 * side], recv_sem=row_recv.at[3 * side],
                device_id=dev, device_id_type=MESH),
            pltpu.make_async_remote_copy(
                src_ref=su_hbm.at[pl.ds(src_at, HALO), :], dst_ref=hs.at[side],
                send_sem=row_send.at[3 * side + 1], recv_sem=row_recv.at[3 * side + 1],
                device_id=dev, device_id_type=MESH),
        )

    def halo_tile_copy(side):
        dev = (down if side == 0 else up, col)
        src_at = ROWS if side == 0 else HALO
        dst_at = 0 if side == 0 else ROWS + HALO
        return pltpu.make_async_remote_copy(
            src_ref=ht.at[:, pl.ds(src_at, HALO), :], dst_ref=ht.at[:, pl.ds(dst_at, HALO), :],
            send_sem=row_send.at[3 * side + 2], recv_sem=row_recv.at[3 * side + 2],
            device_id=dev, device_id_type=MESH)

    for side in range(2):
        for cp in row_copies(side):
            cp.start()
    for band in (1, 2):
        start_band(band)
        m_copy(band).start()

    def column_halos():
        for side in range(2):
            col_copy(side).wait_recv()

        for b in range(5):
            r = HALO + 128 * b
            src = pl.ds(128 * b, 128)
            for k in range(3):
                tile = jnp.zeros((128, 128), f32)
                for side in range(2):
                    tile = tile + lax.dot_general(
                        inbox[side, :, src], select(side, k), (((0,), (0,)), ((), ())),
                        preferred_element_type=f32)
                ht[k, pl.ds(r, 128), :] = tile
        for side in range(2):
            halo_tile_copy(side).start()

    def part(c):
        return small if c == 0 else large.at[c - 1] if c < 5 else tiny.at[c - 5]

    def y_copy(n, ref):
        _, at, size = SENDS[n]
        return pltpu.make_async_remote_copy(
            src_ref=ref.at[pl.ds(own + at, size)], dst_ref=ref.at[pl.ds(far + at, size)],
            send_sem=ys.at[n], recv_sem=yr.at[n],
            device_id=(row, ycol), device_id_type=MESH)

    def x_copy(n, ref):
        _, at, size = SENDS[n]
        return pltpu.make_async_remote_copy(
            src_ref=ref.at[pl.ds(24 + at, size)], dst_ref=ref.at[pl.ds(8 + at, size)],
            send_sem=xs.at[n], recv_sem=xr.at[n],
            device_id=(row, xcol), device_id_type=MESH)

    def send(keep, n):
        @pl.when(keep == 1)
        def _():
            y_copy(n, part(SENDS[n][0])).start()

        @pl.when(keep == 0)
        def _():
            x_copy(n, part(SENDS[n][0])).start()

    lane = lax.broadcasted_iota(jnp.int32, (8, 128), 1)
    even = lax.rem(lane, 2) == 0
    first, last = lane == 0, lane == 127
    colours = (c0, c1)

    def wrap(ref):
        for t in range(LT + 1):
            ref[0, t] = pltpu.roll(ref[PAIRS, t], 1, 0)
            ref[PAIRS + 1, t] = pltpu.roll(ref[1, t], 7, 0)

    def weigh(ref, keep, row0, start, count, tiles):
        base = own * keep + 24 * (1 - keep)
        for g in range(count // 16):
            at = pl.multiple_of(row0 + start + 16 * g, 16)
            for t in tiles:
                lanes = pl.ds(128 * t, 128)
                w = m[pl.ds(at, 16), lanes] * wk[t, HALO + start + 16 * g:HALO + start + 16 * g + 16, :].astype(bf16)
                ref[base + t // 2, 16 * g:16 * g + 16, 128 * (t % 2):128 * (t % 2 + 1)] = w
                w_ref[pl.ds(at, 16), lanes] = w

    def unit(k, carry):
        p = k - 3 * jnp.minimum(lax.div(k, 3), 1)
        odd = lax.rem(p, 2)
        i = lax.div(p + 1, 2)
        keep = 1 - lax.rem(1 - odd + par, 2)
        row0 = jnp.minimum(jnp.maximum(288 + UNIT * i * (1 - 2 * odd), 0), ROWS - UNIT)

        @pl.when(k == 3)
        def _():
            for n in range(2):
                start_band(3 + n)
            column_halos()

        for n in range(2):
            @pl.when(k == 6 + n)
            def _():
                wait_band(1 + n)
                m_copy(1 + n).wait()

            @pl.when(k == 10 + n)
            def _():
                wait_band(3 + n)

        for side in range(2):
            @pl.when(k == 12 + side)
            def _():
                for cp in row_copies(side):
                    cp.wait_recv()
                halo_tile_copy(side).wait_recv()
                at = 0 if side == 0 else ROWS + HALO
                for t in range(LT):
                    lanes = pl.ds(128 * t, 128)
                    su[t, at:at + HALO, :] = hs[side, :, lanes]
                    for n in range(2):
                        u[n, t, at:at + HALO, :] = hu[side, n, :, lanes]

        for g in range(PAIRS):
            upper = pl.ds(row0 + 2 * g, 8, stride=SPAN)
            lower = pl.ds(row0 + 2 * g + 1, 8, stride=SPAN)
            for t in range(LT + 1):
                if t < LT:
                    a = (2 * su[t, upper, :] - 1).astype(f32)
                    b = (2 * su[t, lower, :] - 1).astype(f32)
                else:
                    a, b = ht[0, upper, :], ht[0, lower, :]
                c0[g + 1, t] = jnp.where(even, a, b)
                c1[g + 1, t] = jnp.where(even, b, a)
        wrap(c1)

        for h in range(4):
            sweep, colour = h // 2, h % 2
            mine, other = colours[colour], colours[1 - colour]

            for g in range(PAIRS):
                upper = pl.ds(row0 + 2 * g + colour, 8, stride=SPAN)
                lower = pl.ds(row0 + 2 * g + 1 - colour, 8, stride=SPAN)
                mid = [other[g + 1, t] for t in range(LT + 1)]
                east = [pltpu.roll(x, 1, 1) for x in mid]
                west = [pltpu.roll(x, 127, 1) for x in mid]
                for t in range(LT + 1):
                    above, below = other[g, t], other[g + 2, t]
                    outer = jnp.where(even, above, below) if colour == 0 else jnp.where(even, below, above)
                    side = (jnp.where(first, east[t - 1], east[t])
                            + jnp.where(last, west[(t + 1) % (LT + 1)], west[t]))
                    if t < LT:
                        bound = limit(jnp.where(even, u[sweep, t, upper, :], u[sweep, t, lower, :]))
                    else:
                        bound = jnp.where(even, ht[1 + sweep, upper, :], ht[1 + sweep, lower, :])
                    cur = mine[g + 1, t]
                    flip = cur * (mid[t] + outer + side) <= bound
                    mine[g + 1, t] = jnp.where(flip, -cur, cur)
            if h < 3:
                wrap(mine)

        for g in range(PAIRS):
            for t in range(LT):
                a, b = c0[g + 1, t], c1[g + 1, t]
                wk[t, pl.ds(2 * g, 8, stride=SPAN), :] = jnp.where(even, a, b)
                wk[t, pl.ds(2 * g + 1, 8, stride=SPAN), :] = jnp.where(even, b, a)

        inner, edges = range(2, LT - 2), (0, 1, LT - 2, LT - 1)
        for late in range(2):
            tiles = edges if late else inner

            @pl.when(k == 3 * late)
            def _():
                for half in range(2):
                    kept = 1 - lax.rem(half + par, 2)
                    weigh(small, kept, row0, 32 * half, 32, tiles)
                    for n in (2, 3) if late else (0,):
                        send(kept, n)

            @pl.when((k >= 1 + 3 * late) & (k < 3 + 3 * late))
            def _():
                weigh(large.at[0], keep, row0, 0, UNIT, tiles)
                for n in (4, 5) if late else (1,):
                    send(keep, n)

        for c in range(1, 4):
            @pl.when((k >= 4 + 2 * c) & (k < 6 + 2 * c))
            def _():
                weigh(large.at[c], keep, row0, 0, UNIT, range(LT))
                send(keep, 5 + c)

        for side in range(2):
            @pl.when(k == 12 + side)
            def _():
                for n in range(2):
                    weigh(tiny.at[n], keep, row0, 16 * (1 - n) if side == 0 else 32 + 16 * n, 16, range(LT))
                    send(keep, 9 + n)

        return carry

    wait_band(0)
    m_copy(0).wait()
    lax.fori_loop(0, 14, unit, 0)

    def chunk(c, height, opening):
        ref = part(c)
        for n, what in enumerate(SENDS):
            if what[0] == c:
                y_copy(n, ref).wait_recv()
                x_copy(n, ref).wait_recv()
        depth = 16 * height
        per = 128 // height
        for n in range(depth // 128):
            rows = ref[per * n:per * n + per].reshape(128, TILE)
            lt[:, 128 * n:128 * (n + 1)] = rows.T
        for o in range(9):
            right = ref[o:o + 16].reshape(depth, TILE)
            p = jnp.dot(lt[:, 0:depth], right, preferred_element_type=f32)
            prod[o] = p if opening else prod[o] + p

    for c, height in enumerate(HEIGHTS):
        chunk(c, height, c == 0)

    for b in range(16):
        r = 8 * b
        lo = jnp.concatenate([prod[o, pl.ds(r, 8), :] for o in range(9)], axis=1)
        hi = jnp.concatenate([prod[o, pl.ds(r + 128, 8), :] for o in range(9)], axis=1)
        fold[pl.ds(r, 8), :] = lo[:, 0:WIDE] + hi[:, 128:128 + WIDE]
    for n in (64, 32, 16, 8):
        for b in range(n // 8):
            r = 8 * b
            fold[pl.ds(r, 8), :] += pltpu.roll(fold[pl.ds(r + n, 8), :], WIDE - n, 1)
    v = fold[0:8, :]
    for n in (4, 2, 1):
        v = v + pltpu.roll(pltpu.roll(v, WIDE - n, 1), 8 - n, 0)

    for i in range(NROW):
        vb[i] = v[0:1, 128 * i:128 * (i + 1)]

    def r1_copy(i):
        to = lax.rem(row + i, NROW)
        return pltpu.make_async_remote_copy(
            src_ref=vb.at[to], dst_ref=rs1.at[i], send_sem=r1s.at[i], recv_sem=r1r.at[i],
            device_id=(to, col), device_id_type=MESH)

    for i in range(1, NROW):
        r1_copy(i).start()
    total = vb[row]
    for i in range(1, NROW):
        r1_copy(i).wait_recv()
        total = total + rs1[i]
    sb[...] = total

    def r2_copy(i):
        return pltpu.make_async_remote_copy(
            src_ref=sb, dst_ref=rs2.at[i], send_sem=r2s.at[i], recv_sem=r2r.at[i],
            device_id=(row, lax.rem(col + i, NCOL)), device_id_type=MESH)

    for i in range(1, NCOL):
        r2_copy(i).start()
    for i in range(1, NCOL):
        r2_copy(i).wait_recv()
        total = total + rs2[i]
    total = total * (1.0 / math.sqrt(ROWS * NROW * CB * NCOL))
    total = pltpu.roll(jnp.broadcast_to(total, (8, 128)), lax.rem(128 - 16 * col, 128), 1)
    corr_ref[...] = total

    for side in range(2):
        col_copy(side).wait_send()
        for cp in row_copies(side):
            cp.wait_send()
        halo_tile_copy(side).wait_send()

    for n, what in enumerate(SENDS):
        y_copy(n, part(what[0])).wait_send()
        x_copy(n, part(what[0])).wait_send()
    for i in range(1, NROW):
        r1_copy(i).wait_send()
    for i in range(1, NCOL):
        r2_copy(i).wait_send()


def finish(w_ref, reduced_ref, spins_hbm, corr_ref, spins, sem):
    block = 64
    copies = []
    for i in range(ROWS // block):
        rows = pl.ds(block * i, block)
        spins[rows, :] = jnp.where(w_ref[rows, :].astype(jnp.float32) > 0, 1.0, -1.0)
        copies.append(pltpu.make_async_copy(spins.at[rows, :], spins_hbm.at[rows, :], sem.at[i]))
        copies[-1].start()
    corr_ref[...] = reduced_ref[0, :16]
    for cp in copies:
        cp.wait()


def on_device(spins_up, uniforms, moments, accept_bar):
    f32, bf16 = jnp.float32, jnp.bfloat16
    vmem, dma = pltpu.VMEM, pltpu.SemaphoreType.DMA
    hbm = pl.BlockSpec(memory_space=pltpu.HBM)
    weighted, corr = pl.pallas_call(
        kernel,
        out_shape=(
            jax.ShapeDtypeStruct((ROWS, CB), bf16),
            jax.ShapeDtypeStruct((8, 128), f32),
        ),
        in_specs=[hbm, hbm, hbm, pl.BlockSpec(memory_space=pltpu.SMEM)],
        out_specs=(pl.BlockSpec(memory_space=pltpu.VMEM), pl.BlockSpec(memory_space=pltpu.VMEM)),
        scratch_shapes=[
            vmem((LT, ROWS + 16, 128), jnp.int32),
            vmem((2, LT, ROWS + 16, 128), f32),
            vmem((2, 2, HALO, CB), f32),
            vmem((2, HALO, CB), jnp.int32),
            vmem((ROWS, CB), bf16),
            vmem((3, ROWS + 16, 128), f32),
            vmem((PAIRS + 2, LT + 1, 8, 128), f32),
            vmem((PAIRS + 2, LT + 1, 8, 128), f32),
            vmem((LT, UNIT + 16, 128), f32),
            vmem((32, 32, TILE), bf16),
            vmem((4, 32, UNIT, TILE), bf16),
            vmem((2, 32, 16, TILE), bf16),
            vmem((TILE, 16 * UNIT), bf16),
            vmem((9, TILE, TILE), f32),
            vmem((128, WIDE), f32),
            vmem((2, 16, ROWS), bf16),
            vmem((2, 16, ROWS), bf16),
            vmem((NROW, 1, 128), f32),
            vmem((NROW, 1, 128), f32),
            vmem((NCOL, 1, 128), f32),
            vmem((1, 128), f32),
            dma((len(BANDS), LT)), dma((len(BANDS), LT)), dma((3,)),
            dma((2,)), dma((2,)), dma((6,)), dma((6,)),
            dma((len(SENDS),)), dma((len(SENDS),)), dma((len(SENDS),)), dma((len(SENDS),)),
            dma((NROW,)), dma((NROW,)), dma((NCOL,)), dma((NCOL,)),
        ],
        compiler_params=pltpu.CompilerParams(
            collective_id=0, has_side_effects=True, vmem_limit_bytes=50 * 1024 * 1024,
        ),
    )(spins_up, uniforms, moments, accept_bar)
    in_vmem = pl.BlockSpec(memory_space=pltpu.VMEM)
    return pl.pallas_call(
        finish,
        out_shape=(
            jax.ShapeDtypeStruct((ROWS, CB), f32),
            jax.ShapeDtypeStruct((16,), f32),
        ),
        in_specs=[in_vmem, in_vmem],
        out_specs=(hbm, in_vmem),
        scratch_shapes=[vmem((ROWS, CB), f32), dma((10,))],
        compiler_params=pltpu.CompilerParams(vmem_limit_bytes=16 * 1024 * 1024),
    )(weighted, corr)


def solution(mesh):
    placed = (P("row", "col"), P(None, "row", "col"), P("row", "col"), P())
    return jax.shard_map(
        on_device,
        mesh=mesh,
        in_specs=placed,
        out_specs=(P("row", "col"), P(("row", "col"))),
        check_vma=False,
    )
```

```python
import math

import jax
import jax.numpy as jnp
from jax import lax
from jax.experimental import pallas as pl
from jax.experimental.pallas import tpu as pltpu
from jax.sharding import PartitionSpec as P

ROWS = 640
CB = 2048
R = 2048
NROW = 16
NCOL = 8
HALO = 8
UNIT = 64
WIDE = CB + 128
TILE = 256
LT = CB // 128
EDGES = (0, LT - 1)
BANDS = ((216, 208), (88, 128), (424, 128), (0, 88), (552, 88), (0, 640))
M_BANDS = ((224, 192), (0, 224), (416, 224))
SENDS = (
    (0, 1, 6), (1, 1, 6), (0, 0, 1), (0, 7, 1), (1, 0, 1), (1, 7, 1),
    (2, 0, 8), (3, 0, 8), (4, 0, 8), (5, 0, 8), (6, 0, 8),
)
HEIGHTS = (32, 64, 64, 64, 64, 16, 16)
SPAN = (UNIT + 2 * HALO) // 8
PAIRS = SPAN // 2
ORDER = sorted(
    ((i, j) for i in range(NROW) for j in range(NCOL) if i or j),
    key=lambda e: (-(2 - abs(2 - e[0] // 2 % 4)) - 2 * (e[0] // 8) - (2 - abs(2 - e[1] // 2)), e),
)
MESH = pl.DeviceIdType.MESH


def kernel(
    su_hbm, u_hbm, m_hbm, bar, w_ref, corr_ref,
    su, u, hu, hs, m, ht, c0, c1, wk, small, large, tiny, lt, prod, fold, outbox, inbox, vb, gathered,
    u_sem, s_sem, m_sem, col_send, col_recv,
    row_send, row_recv, ys, yr, xs, xr, all_send, all_recv, entered,
):
    f32, bf16 = jnp.float32, jnp.bfloat16
    row = lax.axis_index("row")
    col = lax.axis_index("col")
    par = lax.rem(col, 2)
    xcol = col + 1 - 2 * par
    ycol = lax.rem(col + 6 + 4 * par, NCOL)
    left, right = lax.rem(col + NCOL - 1, NCOL), lax.rem(col + 1, NCOL)
    up, down = lax.rem(row + NROW - 1, NROW), lax.rem(row + 1, NROW)
    own = 16 * par
    far = 16 * (1 - par)

    barrier = pltpu.get_barrier_semaphore()
    for i in range(1, NROW):
        pl.semaphore_signal(
            barrier, inc=1, device_id=(lax.rem(row + i, NROW), col), device_id_type=MESH
        )
    for i in range(1, NCOL):
        pl.semaphore_signal(
            barrier, inc=1, device_id=(row, lax.rem(col + i, NCOL)), device_id_type=MESH
        )

    def tile_copies(t, band):
        at, size = BANDS[band]
        lanes = pl.ds(128 * t, 128)
        return (
            pltpu.make_async_copy(
                u_hbm.at[:, pl.ds(at, size), lanes],
                u.at[:, t, pl.ds(at + HALO, size), :], u_sem.at[band, t]),
            pltpu.make_async_copy(
                su_hbm.at[pl.ds(at, size), lanes],
                su.at[t, pl.ds(at + HALO, size), :], s_sem.at[band, t]),
        )

    def m_copy(band):
        rows = pl.ds(*M_BANDS[band])
        return pltpu.make_async_copy(m_hbm.at[rows, :], m.at[rows, :], m_sem.at[band])

    def start_band(band):
        tiles = EDGES if band == 5 else range(1, LT - 1)
        for t in tiles:
            for cp in tile_copies(t, band):
                cp.start()

    def wait_band(band):
        tiles = EDGES if band == 5 else range(1, LT - 1)
        for t in tiles:
            for cp in tile_copies(t, band):
                cp.wait()

    start_band(5)
    start_band(0)
    m_copy(0).start()

    a0 = bar[0]
    a1 = bar[1]

    def limit(draws):
        return jnp.where(draws < a1, 4.0, jnp.where(draws < a0, 2.0, 0.0)).astype(f32)

    def select(side, k):
        r = lax.broadcasted_iota(jnp.int32, (16, 128), 0)
        c = lax.broadcasted_iota(jnp.int32, (16, 128), 1)
        c = c - 124 * side
        hit = (c >= 0) & (c < 4) & (r == 4 * k + c)
        return jnp.where(hit, 1.0, 0.0).astype(bf16)

    for n in range(3):
        for b in range(5):
            ht[n, HALO + 128 * b:HALO + 128 * (b + 1), :] = jnp.zeros((128, 128), f32)
    wait_band(5)

    for b in range(5):
        r = HALO + 128 * b
        dst = pl.ds(128 * b, 128)
        for side in range(2):
            t = EDGES[side]
            parts = (
                (2 * su[t, pl.ds(r, 128), :] - 1).astype(f32),
                limit(u[0, t, pl.ds(r, 128), :]),
                limit(u[1, t, pl.ds(r, 128), :]),
            )
            msg = jnp.zeros((16, 128), f32)
            for k, x in enumerate(parts):
                msg = msg + lax.dot_general(
                    select(side, k), x.astype(bf16), (((1,), (1,)), ((), ())),
                    preferred_element_type=f32)
            outbox[side, :, dst] = msg.astype(bf16)

    pl.semaphore_wait(barrier, NROW + NCOL - 2)
    for i in range(1, NCOL):
        pl.semaphore_signal(
            entered, inc=1, device_id=(row, lax.rem(col + i, NCOL)), device_id_type=MESH
        )

    def col_copy(side):
        return pltpu.make_async_remote_copy(
            src_ref=outbox.at[side], dst_ref=inbox.at[side],
            send_sem=col_send.at[side], recv_sem=col_recv.at[side],
            device_id=(row, left if side == 0 else right), device_id_type=MESH)

    for side in range(2):
        col_copy(side).start()

    def row_copies(side):
        dev = (down if side == 0 else up, col)
        src_at = ROWS - HALO if side == 0 else 0
        return (
            pltpu.make_async_remote_copy(
                src_ref=u_hbm.at[:, pl.ds(src_at, HALO), :], dst_ref=hu.at[side],
                send_sem=row_send.at[3 * side], recv_sem=row_recv.at[3 * side],
                device_id=dev, device_id_type=MESH),
            pltpu.make_async_remote_copy(
                src_ref=su_hbm.at[pl.ds(src_at, HALO), :], dst_ref=hs.at[side],
                send_sem=row_send.at[3 * side + 1], recv_sem=row_recv.at[3 * side + 1],
                device_id=dev, device_id_type=MESH),
        )

    def halo_tile_copy(side):
        dev = (down if side == 0 else up, col)
        src_at = ROWS if side == 0 else HALO
        dst_at = 0 if side == 0 else ROWS + HALO
        return pltpu.make_async_remote_copy(
            src_ref=ht.at[:, pl.ds(src_at, HALO), :], dst_ref=ht.at[:, pl.ds(dst_at, HALO), :],
            send_sem=row_send.at[3 * side + 2], recv_sem=row_recv.at[3 * side + 2],
            device_id=dev, device_id_type=MESH)

    for side in range(2):
        for cp in row_copies(side):
            cp.start()
    for band in (1, 2):
        start_band(band)
        m_copy(band).start()

    def column_halos():
        for side in range(2):
            col_copy(side).wait_recv()

        for b in range(5):
            r = HALO + 128 * b
            src = pl.ds(128 * b, 128)
            for k in range(3):
                tile = jnp.zeros((128, 128), f32)
                for side in range(2):
                    tile = tile + lax.dot_general(
                        inbox[side, :, src], select(side, k), (((0,), (0,)), ((), ())),
                        preferred_element_type=f32)
                ht[k, pl.ds(r, 128), :] = tile
        for side in range(2):
            halo_tile_copy(side).start()

    def part(c):
        return small if c == 0 else large.at[c - 1] if c < 5 else tiny.at[c - 5]

    def y_copy(n, ref):
        _, at, size = SENDS[n]
        return pltpu.make_async_remote_copy(
            src_ref=ref.at[pl.ds(own + at, size)], dst_ref=ref.at[pl.ds(far + at, size)],
            send_sem=ys.at[n], recv_sem=yr.at[n],
            device_id=(row, ycol), device_id_type=MESH)

    def x_copy(n, ref):
        _, at, size = SENDS[n]
        return pltpu.make_async_remote_copy(
            src_ref=ref.at[pl.ds(24 + at, size)], dst_ref=ref.at[pl.ds(8 + at, size)],
            send_sem=xs.at[n], recv_sem=xr.at[n],
            device_id=(row, xcol), device_id_type=MESH)

    def send(keep, n):
        @pl.when(keep == 1)
        def _():
            y_copy(n, part(SENDS[n][0])).start()

        @pl.when(keep == 0)
        def _():
            x_copy(n, part(SENDS[n][0])).start()

    lane = lax.broadcasted_iota(jnp.int32, (8, 128), 1)
    even = lax.rem(lane, 2) == 0
    first, last = lane == 0, lane == 127
    colours = (c0, c1)

    def wrap(ref):
        for t in range(LT + 1):
            ref[0, t] = pltpu.roll(ref[PAIRS, t], 1, 0)
            ref[PAIRS + 1, t] = pltpu.roll(ref[1, t], 7, 0)

    def weigh(ref, keep, row0, start, count, tiles):
        base = own * keep + 24 * (1 - keep)
        for g in range(count // 16):
            at = pl.multiple_of(row0 + start + 16 * g, 16)
            for t in tiles:
                lanes = pl.ds(128 * t, 128)
                w = m[pl.ds(at, 16), lanes] * wk[t, HALO + start + 16 * g:HALO + start + 16 * g + 16, :].astype(bf16)
                ref[base + t // 2, 16 * g:16 * g + 16, 128 * (t % 2):128 * (t % 2 + 1)] = w
                w_ref[pl.ds(at, 16), lanes] = w

    def unit(k, carry):
        p = k - 3 * jnp.minimum(lax.div(k, 3), 1)
        odd = lax.rem(p, 2)
        i = lax.div(p + 1, 2)
        keep = 1 - lax.rem(1 - odd + par, 2)
        row0 = jnp.minimum(jnp.maximum(288 + UNIT * i * (1 - 2 * odd), 0), ROWS - UNIT)

        @pl.when(k == 3)
        def _():
            for n in range(2):
                start_band(3 + n)
            column_halos()

        for n in range(2):
            @pl.when(k == 6 + n)
            def _():
                wait_band(1 + n)
                m_copy(1 + n).wait()

            @pl.when(k == 10 + n)
            def _():
                wait_band(3 + n)

        for side in range(2):
            @pl.when(k == 12 + side)
            def _():
                for cp in row_copies(side):
                    cp.wait_recv()
                halo_tile_copy(side).wait_recv()
                at = 0 if side == 0 else ROWS + HALO
                for t in range(LT):
                    lanes = pl.ds(128 * t, 128)
                    su[t, at:at + HALO, :] = hs[side, :, lanes]
                    for n in range(2):
                        u[n, t, at:at + HALO, :] = hu[side, n, :, lanes]

        for g in range(PAIRS):
            upper = pl.ds(row0 + 2 * g, 8, stride=SPAN)
            lower = pl.ds(row0 + 2 * g + 1, 8, stride=SPAN)
            for t in range(LT + 1):
                if t < LT:
                    a = (2 * su[t, upper, :] - 1).astype(f32)
                    b = (2 * su[t, lower, :] - 1).astype(f32)
                else:
                    a, b = ht[0, upper, :], ht[0, lower, :]
                c0[g + 1, t] = jnp.where(even, a, b)
                c1[g + 1, t] = jnp.where(even, b, a)
        wrap(c1)

        for h in range(4):
            sweep, colour = h // 2, h % 2
            mine, other = colours[colour], colours[1 - colour]

            for g in range(PAIRS):
                upper = pl.ds(row0 + 2 * g + colour, 8, stride=SPAN)
                lower = pl.ds(row0 + 2 * g + 1 - colour, 8, stride=SPAN)
                mid = [other[g + 1, t] for t in range(LT + 1)]
                east = [pltpu.roll(x, 1, 1) for x in mid]
                west = [pltpu.roll(x, 127, 1) for x in mid]
                for t in range(LT + 1):
                    above, below = other[g, t], other[g + 2, t]
                    outer = jnp.where(even, above, below) if colour == 0 else jnp.where(even, below, above)
                    side = (jnp.where(first, east[t - 1], east[t])
                            + jnp.where(last, west[(t + 1) % (LT + 1)], west[t]))
                    if t < LT:
                        bound = limit(jnp.where(even, u[sweep, t, upper, :], u[sweep, t, lower, :]))
                    else:
                        bound = jnp.where(even, ht[1 + sweep, upper, :], ht[1 + sweep, lower, :])
                    cur = mine[g + 1, t]
                    flip = cur * (mid[t] + outer + side) <= bound
                    mine[g + 1, t] = jnp.where(flip, -cur, cur)
            if h < 3:
                wrap(mine)

        for g in range(PAIRS):
            for t in range(LT):
                a, b = c0[g + 1, t], c1[g + 1, t]
                wk[t, pl.ds(2 * g, 8, stride=SPAN), :] = jnp.where(even, a, b)
                wk[t, pl.ds(2 * g + 1, 8, stride=SPAN), :] = jnp.where(even, b, a)

        inner, edges = range(2, LT - 2), (0, 1, LT - 2, LT - 1)
        for late in range(2):
            tiles = edges if late else inner

            @pl.when(k == 3 * late)
            def _():
                for half in range(2):
                    kept = 1 - lax.rem(half + par, 2)
                    weigh(small, kept, row0, 32 * half, 32, tiles)
                    for n in (2, 3) if late else (0,):
                        send(kept, n)

            @pl.when((k >= 1 + 3 * late) & (k < 3 + 3 * late))
            def _():
                weigh(large.at[0], keep, row0, 0, UNIT, tiles)
                for n in (4, 5) if late else (1,):
                    send(keep, n)

        for c in range(1, 4):
            @pl.when((k >= 4 + 2 * c) & (k < 6 + 2 * c))
            def _():
                weigh(large.at[c], keep, row0, 0, UNIT, range(LT))
                send(keep, 5 + c)

        for side in range(2):
            @pl.when(k == 12 + side)
            def _():
                for n in range(2):
                    weigh(tiny.at[n], keep, row0, 16 * (1 - n) if side == 0 else 32 + 16 * n, 16, range(LT))
                    send(keep, 9 + n)

        return carry

    wait_band(0)
    m_copy(0).wait()
    lax.fori_loop(0, 14, unit, 0)

    def chunk(c, height, opening):
        ref = part(c)
        for n, what in enumerate(SENDS):
            if what[0] == c:
                y_copy(n, ref).wait_recv()
                x_copy(n, ref).wait_recv()
        depth = 16 * height
        per = 128 // height
        for n in range(depth // 128):
            rows = ref[per * n:per * n + per].reshape(128, TILE)
            lt[:, 128 * n:128 * (n + 1)] = rows.T
        for o in range(9):
            right = ref[o:o + 16].reshape(depth, TILE)
            p = jnp.dot(lt[:, 0:depth], right, preferred_element_type=f32)
            prod[o] = p if opening else prod[o] + p

    for c, height in enumerate(HEIGHTS):
        chunk(c, height, c == 0)

    for b in range(16):
        r = 8 * b
        lo = jnp.concatenate([prod[o, pl.ds(r, 8), :] for o in range(9)], axis=1)
        hi = jnp.concatenate([prod[o, pl.ds(r + 128, 8), :] for o in range(9)], axis=1)
        fold[pl.ds(r, 8), :] = lo[:, 0:WIDE] + hi[:, 128:128 + WIDE]
    for n in (64, 32, 16, 8):
        for b in range(n // 8):
            r = 8 * b
            fold[pl.ds(r, 8), :] += pltpu.roll(fold[pl.ds(r + n, 8), :], WIDE - n, 1)
    v = fold[0:8, :]
    for n in (4, 2, 1):
        v = v + pltpu.roll(pltpu.roll(v, WIDE - n, 1), 8 - n, 0)

    for i in range(NROW):
        vb[i] = v[0:1, 128 * i:128 * (i + 1)]

    to_row = [lax.rem(row + i, NROW) for i in range(NROW)]
    to_col = [lax.rem(col + i, NCOL) for i in range(NCOL)]
    pl.semaphore_wait(entered, NCOL - 1)
    for i, j in ORDER:
        pltpu.make_async_remote_copy(
            src_ref=vb.at[to_row[i]], dst_ref=gathered.at[NCOL * i + j],
            send_sem=all_send.at[0], recv_sem=all_recv.at[0],
            device_id=(to_row[i], to_col[j]), device_id_type=MESH).start()
    others = gathered.at[pl.ds(1, NROW * NCOL - 1)]
    every = pltpu.make_async_remote_copy(
        src_ref=others, dst_ref=others, send_sem=all_send.at[0], recv_sem=all_recv.at[0],
        device_id=(row, right), device_id_type=MESH)
    every.wait_recv()
    sums = [vb[row]] + [gathered[i] for i in range(1, 8)]
    for i in range(8, NROW * NCOL):
        sums[i % 8] = sums[i % 8] + gathered[i]
    total = sum(sums[1:], sums[0])
    total = total * (1.0 / math.sqrt(ROWS * NROW * CB * NCOL))
    total = pltpu.roll(jnp.broadcast_to(total, (8, 128)), lax.rem(128 - 16 * col, 128), 1)
    corr_ref[...] = total

    for side in range(2):
        col_copy(side).wait_send()
        for cp in row_copies(side):
            cp.wait_send()
        halo_tile_copy(side).wait_send()

    for n, what in enumerate(SENDS):
        y_copy(n, part(what[0])).wait_send()
        x_copy(n, part(what[0])).wait_send()
    every.wait_send()


def finish(w_ref, reduced_ref, spins_hbm, corr_ref, spins, sem):
    block = 64
    copies = []
    for i in range(ROWS // block):
        rows = pl.ds(block * i, block)
        spins[rows, :] = jnp.where(w_ref[rows, :].astype(jnp.float32) > 0, 1.0, -1.0)
        copies.append(pltpu.make_async_copy(spins.at[rows, :], spins_hbm.at[rows, :], sem.at[i]))
        copies[-1].start()
    corr_ref[...] = reduced_ref[0, :16]
    for cp in copies:
        cp.wait()


def on_device(spins_up, uniforms, moments, accept_bar):
    f32, bf16 = jnp.float32, jnp.bfloat16
    vmem, dma = pltpu.VMEM, pltpu.SemaphoreType.DMA
    hbm = pl.BlockSpec(memory_space=pltpu.HBM)
    weighted, corr = pl.pallas_call(
        kernel,
        out_shape=(
            jax.ShapeDtypeStruct((ROWS, CB), bf16),
            jax.ShapeDtypeStruct((8, 128), f32),
        ),
        in_specs=[hbm, hbm, hbm, pl.BlockSpec(memory_space=pltpu.SMEM)],
        out_specs=(pl.BlockSpec(memory_space=pltpu.VMEM), pl.BlockSpec(memory_space=pltpu.VMEM)),
        scratch_shapes=[
            vmem((LT, ROWS + 16, 128), jnp.int32),
            vmem((2, LT, ROWS + 16, 128), f32),
            vmem((2, 2, HALO, CB), f32),
            vmem((2, HALO, CB), jnp.int32),
            vmem((ROWS, CB), bf16),
            vmem((3, ROWS + 16, 128), f32),
            vmem((PAIRS + 2, LT + 1, 8, 128), f32),
            vmem((PAIRS + 2, LT + 1, 8, 128), f32),
            vmem((LT, UNIT + 16, 128), f32),
            vmem((32, 32, TILE), bf16),
            vmem((4, 32, UNIT, TILE), bf16),
            vmem((2, 32, 16, TILE), bf16),
            vmem((TILE, 16 * UNIT), bf16),
            vmem((9, TILE, TILE), f32),
            vmem((128, WIDE), f32),
            vmem((2, 16, ROWS), bf16),
            vmem((2, 16, ROWS), bf16),
            vmem((NROW, 1, 128), f32),
            vmem((NROW * NCOL, 1, 128), f32),
            dma((len(BANDS), LT)), dma((len(BANDS), LT)), dma((3,)),
            dma((2,)), dma((2,)), dma((6,)), dma((6,)),
            dma((len(SENDS),)), dma((len(SENDS),)), dma((len(SENDS),)), dma((len(SENDS),)),
            dma((1,)), dma((1,)), pltpu.SemaphoreType.REGULAR,
        ],
        compiler_params=pltpu.CompilerParams(
            collective_id=0, has_side_effects=True, vmem_limit_bytes=50 * 1024 * 1024,
        ),
    )(spins_up, uniforms, moments, accept_bar)
    in_vmem = pl.BlockSpec(memory_space=pltpu.VMEM)
    return pl.pallas_call(
        finish,
        out_shape=(
            jax.ShapeDtypeStruct((ROWS, CB), f32),
            jax.ShapeDtypeStruct((16,), f32),
        ),
        in_specs=[in_vmem, in_vmem],
        out_specs=(hbm, in_vmem),
        scratch_shapes=[vmem((ROWS, CB), f32), dma((10,))],
        compiler_params=pltpu.CompilerParams(vmem_limit_bytes=16 * 1024 * 1024),
    )(weighted, corr)


def solution(mesh):
    placed = (P("row", "col"), P(None, "row", "col"), P("row", "col"), P())
    return jax.shard_map(
        on_device,
        mesh=mesh,
        in_specs=placed,
        out_specs=(P("row", "col"), P(("row", "col"))),
        check_vma=False,
    )
```

```python
import math

import jax
import jax.numpy as jnp
from jax import lax
from jax.experimental import pallas as pl
from jax.experimental.pallas import tpu as pltpu
from jax.sharding import PartitionSpec as P

ROWS = 640
CB = 2048
R = 2048
NROW = 16
NCOL = 8
HALO = 8
UNIT = 64
WIDE = CB + 128
TILE = 256
LT = CB // 128
EDGES = (0, LT - 1)
BANDS = ((216, 208), (88, 128), (424, 128), (0, 88), (552, 88), (0, 640))
M_BANDS = ((224, 192), (0, 224), (416, 224))
SENDS = (
    (0, 1, 6), (1, 1, 6), (0, 0, 1), (0, 7, 1), (1, 0, 1), (1, 7, 1),
    (2, 0, 8), (3, 0, 8), (4, 0, 8), (5, 0, 8), (6, 0, 8),
)
HEIGHTS = (32, 64, 64, 64, 64, 16, 16)
SPAN = (UNIT + 2 * HALO) // 8
PAIRS = SPAN // 2
ORDER = sorted(
    ((i, j) for i in range(NROW) for j in range(NCOL) if i or j),
    key=lambda e: (-(2 - abs(2 - e[0] // 2 % 4)) - 2 * (e[0] // 8) - (2 - abs(2 - e[1] // 2)), e),
)
MESH = pl.DeviceIdType.MESH


def kernel(
    su_hbm, u_hbm, m_hbm, bar, w_ref, corr_ref,
    su, u, hu, hs, m, ht, c0, c1, wk, small, large, tiny, lt, prod, fold, outbox, inbox, vb, gathered,
    u_sem, s_sem, m_sem, col_send, col_recv,
    row_send, row_recv, ys, yr, xs, xr, all_send, all_recv, entered,
):
    f32, bf16 = jnp.float32, jnp.bfloat16
    row = lax.axis_index("row")
    col = lax.axis_index("col")
    par = lax.rem(col, 2)
    xcol = col + 1 - 2 * par
    ycol = lax.rem(col + 6 + 4 * par, NCOL)
    left, right = lax.rem(col + NCOL - 1, NCOL), lax.rem(col + 1, NCOL)
    up, down = lax.rem(row + NROW - 1, NROW), lax.rem(row + 1, NROW)
    own = 16 * par
    far = 16 * (1 - par)

    barrier = pltpu.get_barrier_semaphore()
    for i in range(1, NROW):
        pl.semaphore_signal(
            barrier, inc=1, device_id=(lax.rem(row + i, NROW), col), device_id_type=MESH
        )
    for i in range(1, NCOL):
        pl.semaphore_signal(
            barrier, inc=1, device_id=(row, lax.rem(col + i, NCOL)), device_id_type=MESH
        )

    def tile_copies(t, band):
        at, size = BANDS[band]
        lanes = pl.ds(128 * t, 128)
        return (
            pltpu.make_async_copy(
                u_hbm.at[:, pl.ds(at, size), lanes],
                u.at[:, t, pl.ds(at + HALO, size), :], u_sem.at[band, t]),
            pltpu.make_async_copy(
                su_hbm.at[pl.ds(at, size), lanes],
                su.at[t, pl.ds(at + HALO, size), :], s_sem.at[band, t]),
        )

    def m_copy(band):
        rows = pl.ds(*M_BANDS[band])
        return pltpu.make_async_copy(m_hbm.at[rows, :], m.at[rows, :], m_sem.at[band])

    def start_band(band):
        tiles = EDGES if band == 5 else range(1, LT - 1)
        for t in tiles:
            for cp in tile_copies(t, band):
                cp.start()

    def wait_band(band):
        tiles = EDGES if band == 5 else range(1, LT - 1)
        for t in tiles:
            for cp in tile_copies(t, band):
                cp.wait()

    start_band(5)
    start_band(0)
    m_copy(0).start()

    a0 = bar[0]
    a1 = bar[1]

    def limit(draws):
        return jnp.where(draws < a1, 4.0, jnp.where(draws < a0, 2.0, 0.0)).astype(f32)

    def select(side, k):
        r = lax.broadcasted_iota(jnp.int32, (16, 128), 0)
        c = lax.broadcasted_iota(jnp.int32, (16, 128), 1)
        c = c - 124 * side
        hit = (c >= 0) & (c < 4) & (r == 4 * k + c)
        return jnp.where(hit, 1.0, 0.0).astype(bf16)

    for n in range(3):
        for b in range(5):
            ht[n, HALO + 128 * b:HALO + 128 * (b + 1), :] = jnp.zeros((128, 128), f32)
    wait_band(5)

    for b in range(5):
        r = HALO + 128 * b
        dst = pl.ds(128 * b, 128)
        for side in range(2):
            t = EDGES[side]
            parts = (
                (2 * su[t, pl.ds(r, 128), :] - 1).astype(f32),
                limit(u[0, t, pl.ds(r, 128), :]),
                limit(u[1, t, pl.ds(r, 128), :]),
            )
            msg = jnp.zeros((16, 128), f32)
            for k, x in enumerate(parts):
                msg = msg + lax.dot_general(
                    select(side, k), x.astype(bf16), (((1,), (1,)), ((), ())),
                    preferred_element_type=f32)
            outbox[side, :, dst] = msg.astype(bf16)

    pl.semaphore_wait(barrier, NROW + NCOL - 2)
    for i in range(1, NCOL):
        pl.semaphore_signal(
            entered, inc=1, device_id=(row, lax.rem(col + i, NCOL)), device_id_type=MESH
        )

    def col_copy(side):
        return pltpu.make_async_remote_copy(
            src_ref=outbox.at[side], dst_ref=inbox.at[side],
            send_sem=col_send.at[side], recv_sem=col_recv.at[side],
            device_id=(row, left if side == 0 else right), device_id_type=MESH)

    for side in range(2):
        col_copy(side).start()

    def row_copies(side):
        dev = (down if side == 0 else up, col)
        src_at = ROWS - HALO if side == 0 else 0
        return (
            pltpu.make_async_remote_copy(
                src_ref=u_hbm.at[:, pl.ds(src_at, HALO), :], dst_ref=hu.at[side],
                send_sem=row_send.at[3 * side], recv_sem=row_recv.at[3 * side],
                device_id=dev, device_id_type=MESH),
            pltpu.make_async_remote_copy(
                src_ref=su_hbm.at[pl.ds(src_at, HALO), :], dst_ref=hs.at[side],
                send_sem=row_send.at[3 * side + 1], recv_sem=row_recv.at[3 * side + 1],
                device_id=dev, device_id_type=MESH),
        )

    def halo_tile_copy(side):
        dev = (down if side == 0 else up, col)
        src_at = ROWS if side == 0 else HALO
        dst_at = 0 if side == 0 else ROWS + HALO
        return pltpu.make_async_remote_copy(
            src_ref=ht.at[:, pl.ds(src_at, HALO), :], dst_ref=ht.at[:, pl.ds(dst_at, HALO), :],
            send_sem=row_send.at[3 * side + 2], recv_sem=row_recv.at[3 * side + 2],
            device_id=dev, device_id_type=MESH)

    for side in range(2):
        for cp in row_copies(side):
            cp.start()
    for band in (1, 2):
        start_band(band)
        m_copy(band).start()

    def column_halos():
        for side in range(2):
            col_copy(side).wait_recv()

        for b in range(5):
            r = HALO + 128 * b
            src = pl.ds(128 * b, 128)
            for k in range(3):
                tile = jnp.zeros((128, 128), f32)
                for side in range(2):
                    tile = tile + lax.dot_general(
                        inbox[side, :, src], select(side, k), (((0,), (0,)), ((), ())),
                        preferred_element_type=f32)
                ht[k, pl.ds(r, 128), :] = tile
        for side in range(2):
            halo_tile_copy(side).start()

    def part(c):
        return small if c == 0 else large.at[c - 1] if c < 5 else tiny.at[c - 5]

    def y_copy(n, ref):
        _, at, size = SENDS[n]
        return pltpu.make_async_remote_copy(
            src_ref=ref.at[pl.ds(own + at, size)], dst_ref=ref.at[pl.ds(far + at, size)],
            send_sem=ys.at[n], recv_sem=yr.at[n],
            device_id=(row, ycol), device_id_type=MESH)

    def x_copy(n, ref):
        _, at, size = SENDS[n]
        return pltpu.make_async_remote_copy(
            src_ref=ref.at[pl.ds(24 + at, size)], dst_ref=ref.at[pl.ds(8 + at, size)],
            send_sem=xs.at[n], recv_sem=xr.at[n],
            device_id=(row, xcol), device_id_type=MESH)

    def send(keep, n):
        @pl.when(keep == 1)
        def _():
            y_copy(n, part(SENDS[n][0])).start()

        @pl.when(keep == 0)
        def _():
            x_copy(n, part(SENDS[n][0])).start()

    lane = lax.broadcasted_iota(jnp.int32, (8, 128), 1)
    even = lax.rem(lane, 2) == 0
    first, last = lane == 0, lane == 127
    colours = (c0, c1)

    def wrap(ref):
        for t in range(LT + 1):
            ref[0, t] = pltpu.roll(ref[PAIRS, t], 1, 0)
            ref[PAIRS + 1, t] = pltpu.roll(ref[1, t], 7, 0)

    def weigh(ref, keep, row0, start, count, tiles):
        base = own * keep + 24 * (1 - keep)
        for g in range(count // 16):
            at = pl.multiple_of(row0 + start + 16 * g, 16)
            for t in tiles:
                lanes = pl.ds(128 * t, 128)
                w = m[pl.ds(at, 16), lanes] * wk[t, HALO + start + 16 * g:HALO + start + 16 * g + 16, :].astype(bf16)
                ref[base + t // 2, 16 * g:16 * g + 16, 128 * (t % 2):128 * (t % 2 + 1)] = w
                w_ref[pl.ds(at, 16), lanes] = w

    def unit(k, carry):
        p = k - 3 * jnp.minimum(lax.div(k, 3), 1)
        odd = lax.rem(p, 2)
        i = lax.div(p + 1, 2)
        keep = 1 - lax.rem(1 - odd + par, 2)
        row0 = jnp.minimum(jnp.maximum(288 + UNIT * i * (1 - 2 * odd), 0), ROWS - UNIT)

        @pl.when(k == 3)
        def _():
            for n in range(2):
                start_band(3 + n)
            column_halos()

        for n in range(2):
            @pl.when(k == 6 + n)
            def _():
                wait_band(1 + n)
                m_copy(1 + n).wait()

            @pl.when(k == 10 + n)
            def _():
                wait_band(3 + n)

        for side in range(2):
            @pl.when(k == 12 + side)
            def _():
                for cp in row_copies(side):
                    cp.wait_recv()
                halo_tile_copy(side).wait_recv()
                at = 0 if side == 0 else ROWS + HALO
                for t in range(LT):
                    lanes = pl.ds(128 * t, 128)
                    su[t, at:at + HALO, :] = hs[side, :, lanes]
                    for n in range(2):
                        u[n, t, at:at + HALO, :] = hu[side, n, :, lanes]

        for g in range(PAIRS):
            upper = pl.ds(row0 + 2 * g, 8, stride=SPAN)
            lower = pl.ds(row0 + 2 * g + 1, 8, stride=SPAN)
            for t in range(LT + 1):
                if t < LT:
                    a = (2 * su[t, upper, :] - 1).astype(f32)
                    b = (2 * su[t, lower, :] - 1).astype(f32)
                else:
                    a, b = ht[0, upper, :], ht[0, lower, :]
                c0[g + 1, t] = jnp.where(even, a, b)
                c1[g + 1, t] = jnp.where(even, b, a)
        wrap(c1)

        for h in range(4):
            sweep, colour = h // 2, h % 2
            mine, other = colours[colour], colours[1 - colour]

            for g in range(PAIRS):
                upper = pl.ds(row0 + 2 * g + colour, 8, stride=SPAN)
                lower = pl.ds(row0 + 2 * g + 1 - colour, 8, stride=SPAN)
                mid = [other[g + 1, t] for t in range(LT + 1)]
                east = [pltpu.roll(x, 1, 1) for x in mid]
                west = [pltpu.roll(x, 127, 1) for x in mid]
                for t in range(LT + 1):
                    above, below = other[g, t], other[g + 2, t]
                    outer = jnp.where(even, above, below) if colour == 0 else jnp.where(even, below, above)
                    side = (jnp.where(first, east[t - 1], east[t])
                            + jnp.where(last, west[(t + 1) % (LT + 1)], west[t]))
                    if t < LT:
                        bound = limit(jnp.where(even, u[sweep, t, upper, :], u[sweep, t, lower, :]))
                    else:
                        bound = jnp.where(even, ht[1 + sweep, upper, :], ht[1 + sweep, lower, :])
                    cur = mine[g + 1, t]
                    flip = cur * (mid[t] + outer + side) <= bound
                    mine[g + 1, t] = jnp.where(flip, -cur, cur)
            if h < 3:
                wrap(mine)

        for g in range(PAIRS):
            for t in range(LT):
                a, b = c0[g + 1, t], c1[g + 1, t]
                wk[t, pl.ds(2 * g, 8, stride=SPAN), :] = jnp.where(even, a, b)
                wk[t, pl.ds(2 * g + 1, 8, stride=SPAN), :] = jnp.where(even, b, a)

        inner, edges = range(2, LT - 2), (0, 1, LT - 2, LT - 1)
        for late in range(2):
            tiles = edges if late else inner

            @pl.when(k == 3 * late)
            def _():
                for half in range(2):
                    kept = 1 - lax.rem(half + par, 2)
                    weigh(small, kept, row0, 32 * half, 32, tiles)
                    for n in (2, 3) if late else (0,):
                        send(kept, n)

            @pl.when((k >= 1 + 3 * late) & (k < 3 + 3 * late))
            def _():
                weigh(large.at[0], keep, row0, 0, UNIT, tiles)
                for n in (4, 5) if late else (1,):
                    send(keep, n)

        for c in range(1, 4):
            @pl.when((k >= 4 + 2 * c) & (k < 6 + 2 * c))
            def _():
                weigh(large.at[c], keep, row0, 0, UNIT, range(LT))
                send(keep, 5 + c)

        for side in range(2):
            @pl.when(k == 12 + side)
            def _():
                for n in range(2):
                    weigh(tiny.at[n], keep, row0, 16 * (1 - n) if side == 0 else 32 + 16 * n, 16, range(LT))
                    send(keep, 9 + n)

        return carry

    wait_band(0)
    m_copy(0).wait()
    lax.fori_loop(0, 14, unit, 0)

    def chunk(c, height, opening):
        ref = part(c)
        for n, what in enumerate(SENDS):
            if what[0] == c:
                y_copy(n, ref).wait_recv()
                x_copy(n, ref).wait_recv()
        depth = 16 * height
        per = 128 // height
        for n in range(depth // 128):
            rows = ref[per * n:per * n + per].reshape(128, TILE)
            lt[:, 128 * n:128 * (n + 1)] = rows.T
        for o in range(9):
            right = ref[o:o + 16].reshape(depth, TILE)
            p = jnp.dot(lt[:, 0:depth], right, preferred_element_type=f32)
            prod[o] = p if opening else prod[o] + p

    for c, height in enumerate(HEIGHTS):
        chunk(c, height, c == 0)

    for b in range(16):
        r = 8 * b
        lo = jnp.concatenate([prod[o, pl.ds(r, 8), :] for o in range(9)], axis=1)
        hi = jnp.concatenate([prod[o, pl.ds(r + 128, 8), :] for o in range(9)], axis=1)
        fold[pl.ds(r, 8), :] = lo[:, 0:WIDE] + hi[:, 128:128 + WIDE]
    for n in (64, 32, 16, 8):
        for b in range(n // 8):
            r = 8 * b
            fold[pl.ds(r, 8), :] += pltpu.roll(fold[pl.ds(r + n, 8), :], WIDE - n, 1)
    v = fold[0:8, :]
    for n in (4, 2, 1):
        v = v + pltpu.roll(pltpu.roll(v, WIDE - n, 1), 8 - n, 0)

    for i in range(NROW):
        vb[i] = v[0:1, 128 * i:128 * (i + 1)]

    to_row = [lax.rem(row + i, NROW) for i in range(NROW)]
    to_col = [lax.rem(col + i, NCOL) for i in range(NCOL)]
    pl.semaphore_wait(entered, NCOL - 1)
    for i, j in ORDER:
        pltpu.make_async_remote_copy(
            src_ref=vb.at[to_row[i]], dst_ref=gathered.at[NCOL * i + j],
            send_sem=all_send.at[0], recv_sem=all_recv.at[0],
            device_id=(to_row[i], to_col[j]), device_id_type=MESH).start()
    others = gathered.at[pl.ds(1, NROW * NCOL - 1)]
    every = pltpu.make_async_remote_copy(
        src_ref=others, dst_ref=others, send_sem=all_send.at[0], recv_sem=all_recv.at[0],
        device_id=(row, right), device_id_type=MESH)
    every.wait_recv()
    sums = [vb[row]] + [gathered[i] for i in range(1, 8)]
    for i in range(8, NROW * NCOL):
        sums[i % 8] = sums[i % 8] + gathered[i]
    total = sum(sums[1:], sums[0])
    total = total * (1.0 / math.sqrt(ROWS * NROW * CB * NCOL))
    total = pltpu.roll(jnp.broadcast_to(total, (8, 128)), lax.rem(128 - 16 * col, 128), 1)
    corr_ref[...] = total

    for side in range(2):
        col_copy(side).wait_send()
        for cp in row_copies(side):
            cp.wait_send()
        halo_tile_copy(side).wait_send()

    for n, what in enumerate(SENDS):
        y_copy(n, part(what[0])).wait_send()
        x_copy(n, part(what[0])).wait_send()
    every.wait_send()


def finish(w_ref, reduced_ref, spins_hbm, corr_ref, spins, sem):
    block = 32

    def copy(i):
        rows = pl.ds(pl.multiple_of(block * i, block), block)
        return pltpu.make_async_copy(spins.at[rows, :], spins_hbm.at[rows, :], sem.at[i])

    def write(i, carry):
        rows = pl.ds(pl.multiple_of(block * i, block), block)
        spins[rows, :] = jnp.where(w_ref[rows, :].astype(jnp.float32) > 0, 1.0, -1.0)
        copy(i).start()
        return carry

    lax.fori_loop(0, ROWS // block, write, 0)
    corr_ref[...] = reduced_ref[0, :16]

    def drain(i, carry):
        copy(i).wait()
        return carry

    lax.fori_loop(0, ROWS // block, drain, 0)


def on_device(spins_up, uniforms, moments, accept_bar):
    f32, bf16 = jnp.float32, jnp.bfloat16
    vmem, dma = pltpu.VMEM, pltpu.SemaphoreType.DMA
    hbm = pl.BlockSpec(memory_space=pltpu.HBM)
    weighted, corr = pl.pallas_call(
        kernel,
        out_shape=(
            jax.ShapeDtypeStruct((ROWS, CB), bf16),
            jax.ShapeDtypeStruct((8, 128), f32),
        ),
        in_specs=[hbm, hbm, hbm, pl.BlockSpec(memory_space=pltpu.SMEM)],
        out_specs=(pl.BlockSpec(memory_space=pltpu.VMEM), pl.BlockSpec(memory_space=pltpu.VMEM)),
        scratch_shapes=[
            vmem((LT, ROWS + 16, 128), jnp.int32),
            vmem((2, LT, ROWS + 16, 128), f32),
            vmem((2, 2, HALO, CB), f32),
            vmem((2, HALO, CB), jnp.int32),
            vmem((ROWS, CB), bf16),
            vmem((3, ROWS + 16, 128), f32),
            vmem((PAIRS + 2, LT + 1, 8, 128), f32),
            vmem((PAIRS + 2, LT + 1, 8, 128), f32),
            vmem((LT, UNIT + 16, 128), f32),
            vmem((32, 32, TILE), bf16),
            vmem((4, 32, UNIT, TILE), bf16),
            vmem((2, 32, 16, TILE), bf16),
            vmem((TILE, 16 * UNIT), bf16),
            vmem((9, TILE, TILE), f32),
            vmem((128, WIDE), f32),
            vmem((2, 16, ROWS), bf16),
            vmem((2, 16, ROWS), bf16),
            vmem((NROW, 1, 128), f32),
            vmem((NROW * NCOL, 1, 128), f32),
            dma((len(BANDS), LT)), dma((len(BANDS), LT)), dma((3,)),
            dma((2,)), dma((2,)), dma((6,)), dma((6,)),
            dma((len(SENDS),)), dma((len(SENDS),)), dma((len(SENDS),)), dma((len(SENDS),)),
            dma((1,)), dma((1,)), pltpu.SemaphoreType.REGULAR,
        ],
        compiler_params=pltpu.CompilerParams(
            collective_id=0, has_side_effects=True, vmem_limit_bytes=50 * 1024 * 1024,
        ),
    )(spins_up, uniforms, moments, accept_bar)
    in_vmem = pl.BlockSpec(memory_space=pltpu.VMEM)
    return pl.pallas_call(
        finish,
        out_shape=(
            jax.ShapeDtypeStruct((ROWS, CB), f32),
            jax.ShapeDtypeStruct((16,), f32),
        ),
        in_specs=[in_vmem, in_vmem],
        out_specs=(hbm, in_vmem),
        scratch_shapes=[vmem((ROWS, CB), f32), dma((20,))],
        compiler_params=pltpu.CompilerParams(vmem_limit_bytes=16 * 1024 * 1024),
    )(weighted, corr)


def solution(mesh):
    placed = (P("row", "col"), P(None, "row", "col"), P("row", "col"), P())
    return jax.shard_map(
        on_device,
        mesh=mesh,
        in_specs=placed,
        out_specs=(P("row", "col"), P(("row", "col"))),
        check_vma=False,
    )
```
